32 devices in a mesh: dp: 1 (over z), fsdp: 4 (over y), sp: 8 (over x, core).
Axes of the slice: x: 4, y: 4, z: 1, core: 2. Of those that a mesh axis runs over, the one named last changes fastest.
The devices are a block of a 4x4x8 slice.
Arguments:
- x_in: bfloat16 [48, 1024, 2048], P(('dp', 'fsdp'), 'sp')
- norm_attn: bfloat16 [2048], P('fsdp')
- w_query: bfloat16 [2048, 2048], P('fsdp')
- w_key: bfloat16 [2048, 2048], P('fsdp')
- w_value: bfloat16 [2048, 2048], P('fsdp')
- w_out: bfloat16 [2048, 2048], P('fsdp')
- norm_mlp: bfloat16 [2048], P('fsdp')
- w_gate: bfloat16 [2048, 5504], P('fsdp')
- w_up: bfloat16 [2048, 5504], P('fsdp')
- w_down: bfloat16 [5504, 2048], P('fsdp')
Outputs:
- output: bfloat16 [48, 1024, 2048], P(('dp', 'fsdp'), 'sp')
All inputs are finite; a program needn't handle non-finite values.
Results may differ from the reference program's by a relative error of at most 0.011195.
Values are sent between devices in bfloat16 or wider.
A program may use at most 768 MiB of HBM per device.

```python
import math
import jax
import jax.numpy as jnp
from jax import lax

MODEL_DIM = 2048
NUM_HEADS = 16
FFN_DIM = 5504
NUM_ROWS = 48
SEQ_SHARDS = 8
SHARD_LEN = 128
QUERY_BLOCK = 32

HEAD_DIM = MODEL_DIM // NUM_HEADS
SEQ_LEN = SEQ_SHARDS * SHARD_LEN
ANCHOR_GAP = 2 * SEQ_SHARDS
NORM_EPS = 1e-5
ROPE_THETA = 5e7
MASK_VALUE = -1e30


def dealt_order(natural):
    lead_rows = natural.shape[0]
    tail_shape = natural.shape[2:]
    token_grid = natural.reshape((lead_rows, SHARD_LEN, SEQ_SHARDS) + tail_shape)
    return jnp.swapaxes(token_grid, 1, 2).reshape((lead_rows, SEQ_LEN) + tail_shape)


def draw_tokens(rng_key):
    key_anchor, key_noise = jax.random.split(rng_key)
    anchors = jax.random.normal(key_anchor, (NUM_ROWS, SEQ_LEN // ANCHOR_GAP + 1, MODEL_DIM), jnp.float32)
    ramp_wts = (jnp.arange(ANCHOR_GAP, dtype=jnp.float32) / ANCHOR_GAP)[None, None, :, None]
    smooth = (1.0 - ramp_wts) * anchors[:, :-1, None, :] + ramp_wts * anchors[:, 1:, None, :]
    smooth = smooth.reshape(NUM_ROWS, SEQ_LEN, MODEL_DIM)
    noise_part = jax.random.normal(key_noise, (NUM_ROWS, SEQ_LEN, MODEL_DIM), jnp.float32)
    return dealt_order(smooth + 0.3 * noise_part).astype(jnp.bfloat16)


def draw_matrix(rng_key, fan_in, fan_out):
    return jax.random.normal(rng_key, (fan_in, fan_out), jnp.float32) * fan_in ** -0.5


def draw_gain(rng_key):
    return jax.random.uniform(rng_key, (MODEL_DIM,), jnp.float32, 0.5, 1.5).astype(jnp.bfloat16)


def setup_inputs(seed: int = 0, part: int = 0) -> dict:
    root_key = jax.random.key(seed)
    shared_keys = jax.random.split(jax.random.fold_in(root_key, 100003), 9)
    query_w = draw_matrix(shared_keys[1], MODEL_DIM, MODEL_DIM)
    key_w = 0.8 * query_w + 0.6 * draw_matrix(shared_keys[2], MODEL_DIM, MODEL_DIM)
    return {
        'x_in': draw_tokens(jax.random.fold_in(root_key, part)),
        'norm_attn': draw_gain(shared_keys[0]),
        'w_query': query_w.astype(jnp.bfloat16),
        'w_key': key_w.astype(jnp.bfloat16),
        'w_value': draw_matrix(shared_keys[3], MODEL_DIM, MODEL_DIM).astype(jnp.bfloat16),
        'w_out': draw_matrix(shared_keys[4], MODEL_DIM, MODEL_DIM).astype(jnp.bfloat16),
        'norm_mlp': draw_gain(shared_keys[5]),
        'w_gate': draw_matrix(shared_keys[6], MODEL_DIM, FFN_DIM).astype(jnp.bfloat16),
        'w_up': draw_matrix(shared_keys[7], MODEL_DIM, FFN_DIM).astype(jnp.bfloat16),
        'w_down': draw_matrix(shared_keys[8], FFN_DIM, MODEL_DIM).astype(jnp.bfloat16),
    }


def rms_norm(hidden, gain):
    hid_f32 = hidden.astype(jnp.float32)
    inv_rms = lax.rsqrt(jnp.mean(hid_f32 * hid_f32, axis=-1, keepdims=True) + NORM_EPS)
    return (hid_f32 * inv_rms * gain.astype(jnp.float32)).astype(jnp.bfloat16)


def apply_rope(proj, angles):
    half_dim = proj.shape[-1] // 2
    lower_half = proj[..., :half_dim]
    upper_half = proj[..., half_dim:]
    cos_tab = jnp.cos(angles)[..., None, :]
    sin_tab = jnp.sin(angles)[..., None, :]
    return jnp.concatenate([lower_half * cos_tab - upper_half * sin_tab, upper_half * cos_tab + lower_half * sin_tab], axis=-1)


def reference(x_in, norm_attn, w_query, w_key, w_value, w_out, norm_mlp, w_gate, w_up, w_down):
    score_scale = HEAD_DIM ** -0.5
    num_blocks = SEQ_LEN // QUERY_BLOCK
    head_shape = (SEQ_LEN, NUM_HEADS, HEAD_DIM)
    seq_idx = jnp.arange(SEQ_LEN, dtype=jnp.int32)
    row_pos = (seq_idx % SHARD_LEN) * SEQ_SHARDS + seq_idx // SHARD_LEN
    inv_freq = jnp.exp(jnp.arange(HEAD_DIM // 2, dtype=jnp.float32) * (-2.0 * math.log(ROPE_THETA) / HEAD_DIM))
    angles = row_pos.astype(jnp.float32)[:, None] * inv_freq[None, :]
    query_pos = row_pos.reshape(num_blocks, QUERY_BLOCK)

    def row_layer(hidden):
        normed = rms_norm(hidden, norm_attn)
        query_rot = apply_rope(jnp.dot(normed, w_query, preferred_element_type=jnp.float32).reshape(head_shape), angles).astype(jnp.bfloat16)
        key_f32 = apply_rope(jnp.dot(normed, w_key, preferred_element_type=jnp.float32).reshape(head_shape), angles).astype(jnp.bfloat16).astype(jnp.float32)
        value_f32 = jnp.dot(normed, w_value, preferred_element_type=jnp.float32).astype(jnp.bfloat16).astype(jnp.float32).reshape(head_shape)

        def block_layer(block_args):
            hid_blk, query_blk, qpos_blk = block_args
            scores = jnp.einsum('qhd,khd->hqk', query_blk.astype(jnp.float32), key_f32) * score_scale
            allowed = row_pos[None, None, :] <= qpos_blk[None, :, None]
            attn_prob = jax.nn.softmax(jnp.where(allowed, scores, MASK_VALUE), axis=-1)
            attn_mix = jnp.einsum('hqk,khd->qhd', attn_prob, value_f32).astype(jnp.bfloat16).reshape(QUERY_BLOCK, MODEL_DIM)
            resid_blk = (hid_blk.astype(jnp.float32) + jnp.dot(attn_mix, w_out, preferred_element_type=jnp.float32)).astype(jnp.bfloat16)
            normed_mlp = rms_norm(resid_blk, norm_mlp)
            gate_act = jax.nn.silu(jnp.dot(normed_mlp, w_gate, preferred_element_type=jnp.float32))
            up_proj = jnp.dot(normed_mlp, w_up, preferred_element_type=jnp.float32)
            hidden_mlp = (gate_act * up_proj).astype(jnp.bfloat16)
            return (resid_blk.astype(jnp.float32) + jnp.dot(hidden_mlp, w_down, preferred_element_type=jnp.float32)).astype(jnp.bfloat16)

        blocks = (hidden.reshape(num_blocks, QUERY_BLOCK, MODEL_DIM), query_rot.reshape(num_blocks, QUERY_BLOCK, NUM_HEADS, HEAD_DIM), query_pos)
        return lax.map(block_layer, blocks).reshape(SEQ_LEN, MODEL_DIM)

    return lax.map(row_layer, x_in)
```

```python
import functools
import math

import jax
import jax.numpy as jnp
from jax import lax
from jax.experimental import pallas as pl
from jax.experimental.pallas import tpu as pltpu
from jax.sharding import PartitionSpec as P

HEAD = 128
EPS = 1e-5
THETA = 5e7
MASKED = -1e30
CB = 256
SUB = 16
MESH = pl.DeviceIdType.MESH
F32 = jnp.float32
BF16 = jnp.bfloat16


def kernel(cfg, x_hbm, gin, cos_t, sin_t, mask_t, wq, wk, wv, wo, wg, wu, wd, out, bq, bo, bg, bd, H, B, U, OST, QS, KS, VS, W, FA, FO, G, XC, YC, XN,
           rsem, ssem, gsem, gssem, asem, assem, fasem, fassem, shsem, osem, ossem, fosem, fossem, wsem, xcsem, ycsem, xnsem):
    nf, nx, D, F, ROWS, NRB, NS = cfg
    RC = ROWS // nx
    NHG = D // CB
    q4 = NHG // 2
    y = lax.axis_index("fsdp")
    s = lax.axis_index("sp")
    x = s // 2
    c = s % 2
    par = x % 2

    def dev(xx, cc):
        return {"sp": 2 * ((xx + nx) % nx) + cc}

    def ydev(d):
        return {"fsdp": (y + d + nf) % nf}

    sib = {"sp": 2 * x + 1 - c}

    def rcopy(src, dst, ssem_, rsem_, to):
        pltpu.make_async_remote_copy(src_ref=src, dst_ref=dst, send_sem=ssem_, recv_sem=rsem_, device_id=to, device_id_type=MESH).start()

    def wait(view, sem):
        pltpu.make_async_copy(view, view, sem).wait()

    NGU = pl.cdiv(F, CB)
    RD, RF = D // nf, F // nf
    classes = []
    base = 0
    for ws, buf, R, n, two, look in (
        ((wq, wk, wv), bq, RD, NHG, False, 2),
        ((wo,), bo, RD, NHG, False, 3),
        ((wg, wu), bg, RD, NGU, True, 3),
        ((wd,), bd, RF, NHG, True, 3),
    ):
        nr = R // 4 if two else R // 2
        ra = ((nr // 8 + 1) // 2) * 8
        p0 = pl.multiple_of((2 * par + c) * nr if two else c * nr, 8)
        q0 = pl.multiple_of((2 * (1 - par) + c) * nr, 8) if two else None
        ncols = ws[0].shape[1]
        classes.append(dict(ws=ws, buf=buf, R=R, n=n, base=base, two=two, look=look, nr=nr, ra=ra, p0=p0, q0=q0, ncols=ncols, ci=len(classes)))
        base += n
    NSTEP = base
    HGc, Oc, GUc, DNc = classes

    def col0(k, j):
        return pl.multiple_of(jnp.minimum(j * CB, k["ncols"] - CB), 128)

    def each(it, shift, f):
        for k in classes:
            j = it + shift(k) - k["base"]

            @pl.when((j >= 0) & (j < k["n"]))
            def _(k=k, j=j):
                f(k, j)

    def s1_send(k, j):
        rows = pl.ds(k["p0"], k["nr"])
        cols = pl.ds(col0(k, j), CB)
        for wi, w in enumerate(k["ws"]):
            src = w.at[rows, cols]
            rcopy(src, k["buf"].at[j, wi, 2, rows], ssem.at[k["ci"], 0], rsem.at[k["base"] + j, 0], ydev(1))
            rcopy(src, k["buf"].at[j, wi, 0, rows], ssem.at[k["ci"], 0], rsem.at[k["base"] + j, 0], ydev(-1))

    def s1_done(k, j):
        b, ra, nr = k["buf"], k["ra"], k["nr"]
        wait(b.at[j, :, pl.ds(0, 2), pl.ds(k["p0"], nr)], rsem.at[k["base"] + j, 0])
        A = pl.ds(k["p0"], ra)
        Z = pl.ds(pl.multiple_of(k["p0"] + ra, 8), nr - ra)
        rcopy(b.at[j, :, 2, A], b.at[j, :, 1, A], ssem.at[k["ci"], 1], rsem.at[k["base"] + j, 1], ydev(1))
        rcopy(b.at[j, :, 0, Z], b.at[j, :, 1, Z], ssem.at[k["ci"], 1], rsem.at[k["base"] + j, 1], ydev(-1))

    def s2_done(k, j):
        b, ra, nr = k["buf"], k["ra"], k["nr"]
        wait(b.at[j, :, 1, pl.ds(k["p0"], nr)], rsem.at[k["base"] + j, 1])
        rows = pl.ds(k["p0"], nr)
        if k["two"]:
            A = pl.ds(k["p0"], ra)
            Z = pl.ds(pl.multiple_of(k["p0"] + ra, 8), nr - ra)
            rcopy(b.at[j, :, :, A], b.at[j, :, :, A], ssem.at[k["ci"], 2], rsem.at[k["base"] + j, 2], dev(x + 1, c))
            rcopy(b.at[j, :, :, Z], b.at[j, :, :, Z], ssem.at[k["ci"], 2], rsem.at[k["base"] + j, 2], dev(x - 1, c))
        rcopy(b.at[j, :, :, rows], b.at[j, :, :, rows], ssem.at[k["ci"], 3], rsem.at[k["base"] + j, 3], sib)

    def x_done(k, j):
        if k["two"]:
            b = k["buf"]
            rows = pl.ds(k["q0"], k["nr"])
            wait(b.at[j, :, :, rows], rsem.at[k["base"] + j, 2])
            rcopy(b.at[j, :, :, rows], b.at[j, :, :, rows], ssem.at[k["ci"], 3], rsem.at[k["base"] + j, 3], sib)

    def d_wait(k, j):
        wait(k["buf"].at[j, :, :, pl.ds(0, k["R"] // 2)], rsem.at[k["base"] + j, 3])

    def w_load(k, j, slot):
        R = k["R"]
        for wi, w in enumerate(k["ws"]):
            o = wi * nf * R
            pltpu.make_async_copy(w.at[:, pl.ds(col0(k, j), CB)], W.at[slot, pl.ds(pl.multiple_of(o + y * R, 8), R)], wsem.at[slot]).start()
            for r in range(1, nf):
                yy = (y + r) % nf
                pltpu.make_async_copy(k["buf"].at[j, wi, r - 1], W.at[slot, pl.ds(pl.multiple_of(o + yy * R, 8), R)], wsem.at[slot]).start()

    def w_wait(k, slot):
        wait(W.at[slot, pl.ds(0, len(k["ws"]) * nf * k["R"])], wsem.at[slot])

    bar = pltpu.get_barrier_semaphore()
    peers = [ydev(d) for d in range(1, nf)] + [dev(x + 1, 0), dev(x + 1, 1), dev(x - 1, 0), dev(x - 1, 1), sib]
    for p in peers:
        pl.semaphore_signal(bar, inc=1, device_id=p, device_id_type=MESH)
    pl.semaphore_wait(bar, len(peers))

    gcols = pl.ds(pl.multiple_of(y * RD, 128), RD)
    for d in range(1, nf):
        rcopy(gin, G.at[:, gcols], gssem, gsem, ydev(d))
    for i in range(HGc["look"]):
        s1_send(HGc, i)
    G[:, gcols] = gin[...]

    def xn_load(n):
        r = RC * ((x + nx + 2 - n % nx) % nx) + n // nx
        return pltpu.make_async_copy(x_hbm.at[r], XN.at[n % 2], xnsem.at[n % 2])

    xn_load(0).start()
    wait(G.at[:, pl.ds(0, (nf - 1) * RD)], gsem)

    def av(k, src):
        return U.at[pl.ds(0, NRB), src, :, pl.ds(pl.multiple_of(k * D, 128), D)]

    def rms(src, dst, grow, extra=None):
        g = G[pl.ds(grow, 1), :]

        def one(i, carry):
            h = src[i].astype(F32)
            inv = lax.rsqrt(jnp.mean(h * h, axis=-1, keepdims=True) + EPS)
            a = (h * inv * g).astype(BF16)
            dst[i] = a
            return carry

        lax.fori_loop(0, NRB, one, 0, unroll=2)

    def norm_row(n, carry):
        k = n // nx
        d = (nx + 2 - n % nx) % nx
        xd = (x + d) % nx
        r = RC * xd + k
        xn_load(n).wait()

        @pl.when(n + 1 < ROWS)
        def _():
            xn_load(n + 1).start()

        rms(XN.at[n % 2], H.at[r], 0)
        src = H.at[r]

        @pl.when((d == 1) | (d == nx - 1))
        def _():
            @pl.when(k < 2)
            def _():
                rcopy(src, av(0, s), assem, asem.at[0], dev(xd, k))

            @pl.when(k == 2)
            def _():
                rcopy(src, av(1, s), assem, asem.at[1], dev(xd, c))

        @pl.when(d == 2)
        def _():
            rcopy(src, FA.at[k], assem, fasem.at[k], dev(x + 1 - 2 * c, c))

        @pl.when((d == 0) & (k == 1 - c))
        def _():
            rcopy(src, av(0, s), assem, asem.at[0], sib)

        @pl.when((d == 0) & (k == 2))
        def _():
            rcopy(src, av(1, s), assem, asem.at[2], sib)

        @pl.when((d == 0) & ((k == c) | (k == 2)))
        def _():
            kk = k // 2
            U[pl.ds(0, NRB), s, :, pl.ds(pl.multiple_of(kk * D, 128), D)] = H[r]

        return carry

    lax.fori_loop(0, ROWS, norm_row, 0)

    def unit(n):
        m = n - q4
        odd = (n >= q4) & (m % 2 == 1)
        kk = jnp.where(odd, 1, 0)
        hg = jnp.where(odd, 2 * (m // 2) + c, jnp.where(n < q4, n, q4 + m // 2))
        return kk, hg

    def unit_row(kk, xx):
        return RC * ((xx + nx) % nx) + jnp.where(kk == 1, 2, c)

    def unit_load(n):
        kk, hg = unit(n)

        @pl.when(kk == 0)
        def _():
            d_wait(HGc, hg)

        w_load(HGc, hg, n % 2)

    QT = 2 * NS * SUB
    NQT = NRB // 2
    scale2 = (HEAD ** -0.5) * math.log2(math.e)

    def unit_run(n, carry):
        kk, hg = unit(n)
        slot = n % 2
        hcols = pl.ds(pl.multiple_of(hg * CB, CB), CB)

        @pl.when(n == 0)
        def _():
            wait(U.at[pl.ds(0, NRB - 1), :, :, pl.ds(0, D)], asem.at[0])

        @pl.when(n == q4 + 1)
        def _():
            wait(U.at[pl.ds(0, NRB // 2), :, :, pl.ds(0, D)], asem.at[2])

        w_wait(HGc, slot)

        def proj(t, cr):
            rows = pl.ds(pl.multiple_of(t * QT, QT), QT)
            a = U[pl.ds(t * 2, 2), :, :, pl.ds(pl.multiple_of(kk * D, 128), D)].reshape(QT, D)
            cs = cos_t[rows, :]
            sn = sin_t[rows, :]
            for wi, dst in enumerate((QS, KS)):
                p = jnp.dot(a, W[slot, pl.ds(wi * D, D), :], preferred_element_type=F32)
                for h in range(CB // HEAD):
                    ph = p[:, h * HEAD:(h + 1) * HEAD]
                    dst[rows, h * HEAD:(h + 1) * HEAD] = (ph * cs + pltpu.roll(ph, HEAD // 2, 1) * sn).astype(BF16)
            VS[rows, :] = jnp.dot(a, W[slot, pl.ds(2 * D, D), :], preferred_element_type=F32).astype(BF16)
            return cr

        lax.fori_loop(0, NQT, proj, 0)

        @pl.when(n + 1 < 3 * q4)
        def _():
            unit_load(n + 1)

        def head(h, cr):
            hc = pl.ds(pl.multiple_of(h * HEAD, HEAD), HEAD)
            for t in range(NQT):
                kl = (t + 1) * QT
                sc = lax.dot_general(QS[pl.ds(t * QT, QT), hc], KS[pl.ds(0, kl), hc], (((1,), (1,)), ((), ())), preferred_element_type=F32)
                diag = jnp.where(mask_t[...] > 0.0, sc[:, t * QT:], MASKED)
                if t:
                    sc = jnp.concatenate([sc[:, :t * QT], diag], axis=1)
                else:
                    sc = diag
                mx = jnp.max(sc, axis=-1, keepdims=True)
                p = jnp.exp2((sc - mx) * scale2)
                ls = jnp.sum(p, axis=-1, keepdims=True)
                o = jnp.dot(p.astype(BF16), VS[pl.ds(0, kl), hc], preferred_element_type=F32)
                o = (o * (1.0 / ls)).astype(BF16)
                OST[n, pl.ds(2 * t, 2), :, :, hc] = o.reshape(2, NS, SUB, HEAD)
            return cr

        lax.fori_loop(0, CB // HEAD, head, 0)

        row = unit_row(kk, x)
        B[row, :, :, hcols] = OST[n, :, s]
        rcopy(OST.at[n, :, 2 * x + 1 - c], B.at[row, :, :, hcols], ossem.at[n], osem.at[row], sib)
        far = (x + 2) % nx
        rcopy(OST.at[n, :, pl.ds(2 * far, 2)], FO.at[n], ossem.at[n], fosem.at[n], dev(x + 1 - 2 * c, c))
        for dx in (1, nx - 1):
            for cc in range(2):
                xd = (x + dx) % nx
                rcopy(OST.at[n, :, 2 * xd + cc], B.at[row, :, :, hcols], ossem.at[n], osem.at[row], dev(xd, cc))
        return carry

    def unit_forward(n, carry):
        kk, hg = unit(n)
        wait(FO.at[n], fosem.at[n])
        row = unit_row(kk, x - 1 + 2 * c)
        for cc in range(2):
            rcopy(FO.at[n, :, cc], B.at[row, :, :, pl.ds(pl.multiple_of(hg * CB, CB), CB)], fossem.at[n], osem.at[row], dev(x + 1 - 2 * c, cc))
        return carry

    def ustart(it):
        late = jnp.minimum(q4 + 2 * (it - q4 - 2), 3 * q4)
        early = jnp.where(it <= 3, 0, jnp.clip(it - 2, 0, q4)) if q4 > 2 else jnp.clip(it - 2, 0, q4)
        return jnp.where(it >= q4 + 2, late, early)

    MT = 6
    NMT = ROWS // MT
    TM = MT * NRB * SUB
    NOQ = NHG
    OPI = max(1, NHG // 4)

    def xc_load(j, slot):
        return pltpu.make_async_copy(x_hbm.at[:, :, :, pl.ds(pl.multiple_of(j * CB, CB), CB)], XC.at[slot], xcsem.at[slot])

    def yc_copy(j, slot):
        return pltpu.make_async_copy(YC.at[slot], out.at[:, :, :, pl.ds(pl.multiple_of(j * CB, CB), CB)], ycsem.at[slot])

    def prep(qn):
        for k in (Oc, GUc, DNc):
            j = qn + HGc["n"] - k["base"]

            @pl.when((j >= 0) & (j < k["n"]))
            def _(k=k, j=j):
                d_wait(k, j)
                w_load(k, j, qn % 2)
                if k is Oc:
                    xc_load(j, qn % 2).start()

    def o_step(j):
        slot = j % 2
        w_wait(Oc, slot)
        xc_load(j, slot).wait()
        prep(j + 1)
        cols = pl.ds(pl.multiple_of(j * CB, CB), CB)

        def tile(t, cr):
            rr = pl.ds(t * MT, MT)
            p = jnp.dot(B[rr].reshape(TM, D), W[slot, pl.ds(0, D), :], preferred_element_type=F32)
            h = XC[slot, rr].reshape(TM, CB).astype(F32) + p
            H[rr, :, :, cols] = h.astype(BF16).reshape(MT, NRB, SUB, CB)
            return cr

        lax.fori_loop(0, NMT, tile, 0)

    def gu_step(j):
        qn = Oc["n"] + j
        slot = qn % 2
        w_wait(GUc, slot)
        prep(qn + 1)
        cols = pl.ds(col0(GUc, j), CB)

        def tile(t, cr):
            rr = pl.ds(t * MT, MT)
            b = B[rr].reshape(TM, D)
            g = jnp.dot(b, W[slot, pl.ds(0, D), :], preferred_element_type=F32)
            u = jnp.dot(b, W[slot, pl.ds(D, D), :], preferred_element_type=F32)
            act = g * (1.0 / (1.0 + jnp.exp(-g)))
            U[rr, :, :, cols] = (act * u).astype(BF16).reshape(MT, NRB, SUB, CB)
            return cr

        lax.fori_loop(0, NMT, tile, 0)

    def dn_step(j):
        qn = Oc["n"] + GUc["n"] + j
        slot = qn % 2
        w_wait(DNc, slot)
        prep(qn + 1)
        ys = j % 2

        @pl.when(j >= 2)
        def _():
            yc_copy(j - 2, ys).wait()

        cols = pl.ds(pl.multiple_of(j * CB, CB), CB)

        def tile(t, cr):
            rr = pl.ds(t * MT, MT)
            p = jnp.dot(U[rr].reshape(TM, F), W[slot, pl.ds(0, F), :], preferred_element_type=F32)
            h = H[rr, :, :, cols].reshape(TM, CB).astype(F32) + p
            YC[ys, rr] = h.astype(BF16).reshape(MT, NRB, SUB, CB)
            return cr

        lax.fori_loop(0, NMT, tile, 0)
        yc_copy(j, ys).start()

    LAG = 4
    NIT = NSTEP + LAG
    ogo = GUc["base"]

    def step(it, carry):
        each(it, lambda k: k["look"], s1_send)
        each(it, lambda k: 0, s1_done)
        each(it, lambda k: -1, s2_done)
        each(it, lambda k: -2, x_done)

        @pl.when(it < RC)
        def _():
            wait(FA.at[it], fasem.at[it])
            xs = (x - 1 + 2 * c + nx) % nx
            to = x + 1 - 2 * c

            @pl.when(it < 2)
            def _():
                rcopy(FA.at[it], av(0, 2 * xs + c), fassem, asem.at[0], dev(to, it))

            @pl.when(it == 2)
            def _():
                rcopy(FA.at[it], av(1, 2 * xs + c), fassem, asem.at[1], dev(to, c))

        @pl.when(it == q4 + 1)
        def _():
            wait(U.at[pl.ds(0, nx - 1), :, :, pl.ds(0, D)], asem.at[1])
            for d in range(1, nx):
                src = 2 * ((x + d) % nx) + c
                rcopy(av(1, src), av(1, src), shsem, asem.at[2], sib)

        u0, u1, u2 = ustart(it - 1), ustart(it), ustart(it + 1)
        lax.fori_loop(u0, u1, unit_forward, 0)

        @pl.when((u1 == 0) & (u2 > 0))
        def _():
            unit_load(0)

        lax.fori_loop(u1, u2, unit_run, 0)

        @pl.when(it == ogo)
        def _():
            wait(H.at[pl.ds(0, ROWS - 1)], assem)
            wait(FA, fassem)
            wait(U.at[pl.ds(0, nx - 1), :, :, pl.ds(0, D)], shsem)

            def orow(r, cr):
                k = r % RC

                @pl.when((r // RC != x) | (k == 1 - c))
                def _():
                    wait(B.at[r], osem.at[r])

                @pl.when((r // RC == x) & (k == 2))
                def _():
                    wait(B.at[r, pl.ds(0, NRB // 2)], osem.at[r])

                return cr

            prep(0)
            lax.fori_loop(0, ROWS, orow, 0)

        @pl.when((it >= ogo) & (it < ogo + Oc["n"] // OPI))
        def _():
            def go(i, cr):
                o_step((it - ogo) * OPI + i)
                return cr

            lax.fori_loop(0, OPI, go, 0)

        @pl.when(it == ogo + LAG)
        def _():
            def nrow(r, cr):
                rms(H.at[r], B.at[r], 1)
                return cr

            lax.fori_loop(0, ROWS, nrow, 0)

        @pl.when((it >= GUc["base"] + LAG) & (it < GUc["base"] + LAG + GUc["n"]))
        def _():
            gu_step(it - GUc["base"] - LAG)

        @pl.when((it >= DNc["base"] + LAG) & (it < DNc["base"] + LAG + DNc["n"]))
        def _():
            dn_step(it - DNc["base"] - LAG)

        return carry

    lax.fori_loop(0, NIT, step, 0)

    for j in (DNc["n"] - 2, DNc["n"] - 1):
        yc_copy(j, j % 2).wait()

    def drain(n, cr):
        wait(OST.at[n, :, pl.ds(0, NS - 1)], ossem.at[n])
        wait(FO.at[n], fossem.at[n])
        return cr

    lax.fori_loop(0, 3 * q4, drain, 0)
    wait(G.at[:, pl.ds(0, (nf - 1) * RD)], gssem)
    for k in classes:
        b, nr = k["buf"], k["nr"]
        wait(b.at[:, :, pl.ds(0, 2), pl.ds(0, nr)], ssem.at[k["ci"], 0])
        wait(b.at[:, :, 1, pl.ds(0, nr)], ssem.at[k["ci"], 1])
        if k["two"]:
            wait(b.at[:, :, :, pl.ds(0, nr)], ssem.at[k["ci"], 2])
        wait(b.at[:, :, :, pl.ds(0, k["R"] // 2)], ssem.at[k["ci"], 3])


def local_layer(x, norm_attn, wq, wk, wv, wo, norm_mlp, wg, wu, wd, *, nf, ns):
    rows, tl, D = x.shape
    F = wg.shape[1]
    nx = ns // 2
    nrb = tl // SUB
    nhg = D // CB
    ngu = -(-F // CB)
    units = 3 * nhg // 2
    rd, rf = D // nf, F // nf
    tok = ns * tl

    idx = jnp.arange(tok, dtype=jnp.int32)
    blk, src, low = idx // (ns * SUB), idx % (ns * SUB) // SUB, idx % SUB
    pos = (blk * SUB + low) * ns + src
    inv_freq = jnp.exp(jnp.arange(HEAD // 2, dtype=F32) * (-2.0 * math.log(THETA) / HEAD))
    ang = pos.astype(F32)[:, None] * inv_freq[None, :]
    cs, sn = jnp.cos(ang), jnp.sin(ang)
    cos_t = jnp.concatenate([cs, cs], axis=1)
    sin_t = jnp.concatenate([-sn, sn], axis=1)
    qt = 2 * ns * SUB
    mask_t = (pos[None, :qt] <= pos[:qt, None]).astype(F32)
    gin = jnp.concatenate([norm_attn[None], norm_mlp[None]] + [jnp.zeros((6, rd), norm_attn.dtype)], axis=0).astype(F32)
    x4 = x.reshape(rows, nrb, SUB, D)

    nsteps = nhg * 3 + ngu
    dma = pltpu.SemaphoreType.DMA
    anyspec = pl.BlockSpec(memory_space=pl.ANY)
    vspec = pl.BlockSpec(memory_space=pltpu.VMEM)
    outs = [
        jax.ShapeDtypeStruct((rows, nrb, SUB, D), BF16),
        jax.ShapeDtypeStruct((nhg, 3, nf - 1, rd, CB), BF16),
        jax.ShapeDtypeStruct((nhg, 1, nf - 1, rd, CB), BF16),
        jax.ShapeDtypeStruct((ngu, 2, nf - 1, rd, CB), BF16),
        jax.ShapeDtypeStruct((nhg, 1, nf - 1, rf, CB), BF16),
    ]
    wrows = max(3 * D, F)
    res = pl.pallas_call(
        functools.partial(kernel, (nf, nx, D, F, rows, nrb, ns)),
        out_shape=outs,
        in_specs=[anyspec, vspec, vspec, vspec, vspec] + [anyspec] * 7,
        out_specs=[anyspec] * 5,
        scratch_shapes=[
            pltpu.VMEM((rows, nrb, SUB, D), BF16),
            pltpu.VMEM((rows, nrb, SUB, D), BF16),
            pltpu.VMEM((rows, nrb, SUB, F), BF16),
            pltpu.VMEM((units, nrb, ns, SUB, CB), BF16),
            pltpu.VMEM((tok, CB), BF16),
            pltpu.VMEM((tok, CB), BF16),
            pltpu.VMEM((tok, CB), BF16),
            pltpu.VMEM((2, wrows, CB), BF16),
            pltpu.VMEM((rows // nx, nrb, SUB, D), BF16),
            pltpu.VMEM((units, nrb, 2, SUB, CB), BF16),
            pltpu.VMEM((8, D), F32),
            pltpu.VMEM((2, rows, nrb, SUB, CB), BF16),
            pltpu.VMEM((2, rows, nrb, SUB, CB), BF16),
            pltpu.VMEM((2, nrb, SUB, D), BF16),
            dma((nsteps, 4)),
            dma((4, 4)),
            dma,
            dma,
            dma((3,)),
            dma,
            dma((rows // nx,)),
            dma,
            dma,
            dma((rows,)),
            dma((units,)),
            dma((units,)),
            dma((units,)),
            dma((2,)),
            dma((2,)),
            dma((2,)),
            dma((2,)),
        ],
        compiler_params=pltpu.CompilerParams(collective_id=0, has_side_effects=True, vmem_limit_bytes=66 * 1000 * 1000),
        cost_estimate=pl.CostEstimate(flops=170_000_000_000, bytes_accessed=400_000_000, transcendentals=0),
        name="layer",
    )(x4, gin, cos_t, sin_t, mask_t, wq, wk, wv, wo, wg, wu, wd)
    return res[0].reshape(rows, tl, D)


def solution(mesh):
    row = P(("dp", "fsdp"), "sp", None)
    wspec = P("fsdp", None)
    gspec = P("fsdp")
    fn = functools.partial(local_layer, nf=mesh.shape["fsdp"], ns=mesh.shape["sp"])
    specs = (row, gspec, wspec, wspec, wspec, wspec, gspec, wspec, wspec, wspec)
    return jax.shard_map(fn, mesh=mesh, in_specs=specs, out_specs=row, check_vma=False)
```

```python
import functools
import math

import jax
import jax.numpy as jnp
import numpy as np
from jax import lax
from jax.experimental import pallas as pl
from jax.experimental.pallas import tpu as pltpu
from jax.sharding import PartitionSpec as P

HEAD = 128
EPS = 1e-5
THETA = 5e7
MASKED = -1e30
CB = 256
SUB = 16
MESH = pl.DeviceIdType.MESH
F32 = jnp.float32
BF16 = jnp.bfloat16

PUMP1 = [0, 1, 2, 4, 6, 9, 12, 14, 15, 17, 19, 20, 21, 22, 23, 24, 25, 26, 27, 28, 29, 31, 32, 33, 34, 36, 37, 39, 40, 42, 44, 46, 48, 50, 52, 54, 56, 58, 61, 64, 67, 69, 72, 75, 78, 81]
PUMP2 = [2, 4, 7, 10, 12, 14, 16, 18, 19, 20, 21, 22, 23, 25, 26, 27, 29, 30, 31, 32, 33, 34, 36, 37, 39, 40, 42, 44, 46, 48, 50, 52, 55, 57, 59, 60, 62, 65, 67, 70, 73, 76, 79, 82, 83, 84]
PUMP3 = [31, 34, 36, 38, 40, 42, 44, 46, 48, 50, 52, 54, 56, 58, 61, 63, 65, 67, 69, 71, 74, 76, 79, 81, 84, 87, 89, 91, 93, 94]
PUMPO = [9, 10, 13, 14, 17, 19, 21, 23, 25, 27, 29]
NPRE = 5
NGAP = 3


def due(p, pumps):
    words = []
    for q in pumps:
        while len(words) <= q // 7:
            words.append(0)
        words[q // 7] += 1 << (4 * (q % 7))
    w = jnp.int32(0)
    for i, v in enumerate(words):
        if v:
            w = jnp.where(p // 7 == i, v, w)
    return lax.shift_right_logical(w, 4 * (p % 7)) % 16


def pump_lists(nstep, nhg, ngu, ndn, nfo, u0, g0, o0, n0, gu0, dn0):
    q4 = nhg // 2
    need = []
    for h in range(nhg):
        n = h if h < q4 else q4 + 2 * (h - q4)
        need.append(u0 + 2 * n - 1)
    need += [g0] + [o0 + j for j in range(nhg - 1)]
    need += [n0 - 1] + [gu0 + 2 * j for j in range(ngu - 1)]
    need += [dn0 - 2] + [dn0 + 2 * j for j in range(ndn - 1)]
    two = 2 * nhg
    if (nstep, nhg) == (len(PUMP1), 8):
        p1, p2, p3, po = PUMP1, PUMP2, PUMP3, PUMPO
    else:
        p1 = [max(0, q - 3) for q in need]
        p2 = [max(0, q - 2) for q in need]
        p3 = [max(0, q - 1) for q in need[two:]]
        po = [u0 + 2 * n + 3 for n in range(nfo)]
    for i in range(nstep):
        last = p3[i - two] if i >= two else p2[i]
        assert p1[i] <= p2[i] <= last <= need[i], (i, p1[i], p2[i], last, need[i])
    assert all(po[n] > u0 + 2 * n + 1 for n in range(nfo)) and po[-1] < o0
    return p1, p2, p3, po


def kernel(cfg, x_hbm, g1, g2, cos_t, sin_t, mask_t, wq, wk, wv, wo, wg, wu, wd, out, bq, bo, bg, bd, H, B, U, OST, QS, KS, VS, W, FA, FO, GL, G, XC, YC, XN,
           rsem, ssem, gsem, gssem, asem, ownsem, assem, fasem, fassem, shsem, osem, ossem, fosem, fossem, wsem, xcsem, ycsem, xnsem, lsem):
    nf, nx, D, F, ROWS, NRB, NS = cfg
    RC = ROWS // nx
    NHG = D // CB
    q4 = NHG // 2
    y = lax.axis_index("fsdp")
    s = lax.axis_index("sp")
    x = s // 2
    c = s % 2
    par = x % 2

    def dev(xx, cc):
        return {"sp": 2 * ((xx + nx) % nx) + cc}

    def ydev(d):
        return {"fsdp": (y + d + nf) % nf}

    sib = {"sp": 2 * x + 1 - c}

    def rcopy(src, dst, ssem_, rsem_, to):
        pltpu.make_async_remote_copy(src_ref=src, dst_ref=dst, send_sem=ssem_, recv_sem=rsem_, device_id=to, device_id_type=MESH).start()

    def wait(view, sem):
        pltpu.make_async_copy(view, view, sem).wait()

    NGU = pl.cdiv(F, CB)
    RD, RF = D // nf, F // nf
    classes = []
    base = 0
    for ws, buf, R, n, two, look in (
        ((wq, wk, wv), bq, RD, NHG, False, 2),
        ((wo,), bo, RD, NHG, False, 2),
        ((wg, wu), bg, RD, NGU, True, 3),
        ((wd,), bd, RF, NHG, True, 2),
    ):
        nr = R // 4 if two else R // 2
        ra = ((nr // 8 + 1) // 2) * 8
        p0 = pl.multiple_of((2 * par + c) * nr if two else c * nr, 8)
        q0 = pl.multiple_of((2 * (1 - par) + c) * nr, 8) if two else None
        ncols = ws[0].shape[1]
        classes.append(dict(ws=ws, buf=buf, R=R, n=n, base=base, two=two, look=look, nr=nr, ra=ra, p0=p0, q0=q0, ncols=ncols, ci=len(classes)))
        base += n
    NSTEP = base
    HGc, Oc, GUc, DNc = classes

    def col0(k, j):
        return pl.multiple_of(jnp.minimum(j * CB, k["ncols"] - CB), 128)

    def each(it, shift, f):
        for k in classes:
            j = it + shift(k) - k["base"]

            @pl.when((j >= 0) & (j < k["n"]))
            def _(k=k, j=j):
                f(k, j)

    def s1_send(k, j):
        rows = pl.ds(k["p0"], k["nr"])
        cols = pl.ds(col0(k, j), CB)
        for wi, w in enumerate(k["ws"]):
            src = w.at[rows, cols]
            rcopy(src, k["buf"].at[j, wi, 2, rows], ssem.at[k["ci"], 0], rsem.at[k["base"] + j, 0], ydev(1))
            rcopy(src, k["buf"].at[j, wi, 0, rows], ssem.at[k["ci"], 0], rsem.at[k["base"] + j, 0], ydev(-1))

    def s1_done(k, j):
        b, ra, nr = k["buf"], k["ra"], k["nr"]
        wait(b.at[j, :, pl.ds(0, 2), pl.ds(k["p0"], nr)], rsem.at[k["base"] + j, 0])
        A = pl.ds(k["p0"], ra)
        Z = pl.ds(pl.multiple_of(k["p0"] + ra, 8), nr - ra)
        rcopy(b.at[j, :, 2, A], b.at[j, :, 1, A], ssem.at[k["ci"], 1], rsem.at[k["base"] + j, 1], ydev(1))
        rcopy(b.at[j, :, 0, Z], b.at[j, :, 1, Z], ssem.at[k["ci"], 1], rsem.at[k["base"] + j, 1], ydev(-1))

    def s2_done(k, j):
        b, ra, nr = k["buf"], k["ra"], k["nr"]
        wait(b.at[j, :, 1, pl.ds(k["p0"], nr)], rsem.at[k["base"] + j, 1])
        rows = pl.ds(k["p0"], nr)
        if k["two"]:
            A = pl.ds(k["p0"], ra)
            Z = pl.ds(pl.multiple_of(k["p0"] + ra, 8), nr - ra)
            rcopy(b.at[j, :, :, A], b.at[j, :, :, A], ssem.at[k["ci"], 2], rsem.at[k["base"] + j, 2], dev(x + 1, c))
            rcopy(b.at[j, :, :, Z], b.at[j, :, :, Z], ssem.at[k["ci"], 2], rsem.at[k["base"] + j, 2], dev(x - 1, c))
        rcopy(b.at[j, :, :, rows], b.at[j, :, :, rows], ssem.at[k["ci"], 3], rsem.at[k["base"] + j, 3], sib)

    def x_done(k, j):
        if k["two"]:
            b = k["buf"]
            rows = pl.ds(k["q0"], k["nr"])
            wait(b.at[j, :, :, rows], rsem.at[k["base"] + j, 2])
            rcopy(b.at[j, :, :, rows], b.at[j, :, :, rows], ssem.at[k["ci"], 3], rsem.at[k["base"] + j, 3], sib)

    def d_wait(k, j):
        wait(k["buf"].at[j, :, :, pl.ds(0, k["R"] // 2)], rsem.at[k["base"] + j, 3])

    def w_load(k, j, slot):
        R = k["R"]
        for wi, w in enumerate(k["ws"]):
            o = wi * nf * R
            pltpu.make_async_copy(w.at[:, pl.ds(col0(k, j), CB)], W.at[slot, pl.ds(pl.multiple_of(o + y * R, 8), R)], wsem.at[slot]).start()
            for r in range(1, nf):
                yy = (y + r) % nf
                pltpu.make_async_copy(k["buf"].at[j, wi, r - 1], W.at[slot, pl.ds(pl.multiple_of(o + yy * R, 8), R)], wsem.at[slot]).start()

    def w_wait(k, slot):
        wait(W.at[slot, pl.ds(0, len(k["ws"]) * nf * k["R"])], wsem.at[slot])

    GL[...] = jnp.zeros_like(GL)
    GL[0:1, :] = g1[...].astype(F32)
    GL[1:2, :] = g2[...].astype(F32)
    bar = pltpu.get_barrier_semaphore()
    peers = [ydev(d) for d in range(1, nf)] + [dev(x + d, cc) for d in range(1, nx) for cc in range(2)] + [sib]
    for p in peers:
        pl.semaphore_signal(bar, inc=1, device_id=p, device_id_type=MESH)

    def av(k, src):
        return U.at[pl.ds(0, NRB), src, :, pl.ds(pl.multiple_of(k * D, 128), D)]

    def xn_load(i):
        r = RC * ((x + i) % nx) + 2
        return pltpu.make_async_copy(x_hbm.at[r], XN.at[i % 2], xnsem.at[i % 2])

    xn_load(0).start()
    pltpu.make_async_copy(x_hbm.at[RC * x + c], av(0, s), lsem).start()
    with jax.named_scope("bar"):
        pl.semaphore_wait(bar, len(peers))

    gcols = pl.ds(pl.multiple_of(y * RD, 128), RD)
    for d in range(1, nf):
        rcopy(GL, G.at[:, gcols], gssem, gsem, ydev(d))
    for i in range(HGc["look"]):
        s1_send(HGc, i)
    over = dev(x + 1 - 2 * c, c)
    far = (x + 2) % nx
    rcopy(x_hbm.at[RC * x + 1 - c], av(0, s), assem, ownsem.at[0], sib)
    for k in range(2):
        rcopy(x_hbm.at[RC * far + k], FA.at[k], assem, fasem.at[k], over)
    for k in range(2):
        for d in (1, nx - 1):
            rcopy(x_hbm.at[RC * ((x + d) % nx) + k], av(0, s), assem, ownsem.at[nx - d], dev(x + d, k))
    G[:, gcols] = GL[...]
    with jax.named_scope("wg"):
        wait(G.at[:, pl.ds(0, (nf - 1) * RD)], gsem)

    def rms(src, dst, grow):
        g = G[pl.ds(grow, 1), :]

        def one(i, carry):
            h = src[i].astype(F32)
            inv = lax.rsqrt(jnp.mean(h * h, axis=-1, keepdims=True) + EPS)
            dst[i] = (h * inv * g).astype(BF16)
            return carry

        lax.fori_loop(0, NRB, one, 0, unroll=2)

    def norm_shared(i, carry):
        xn_load(i).wait()

        @pl.when(i + 1 < nx)
        def _():
            xn_load(i + 1).start()

        rms(XN.at[i % 2], H.at[i], 0)

        @pl.when(i == 0)
        def _():
            U[pl.ds(0, NRB), s, :, pl.ds(D, D)] = H[0]

        return carry

    def norm_chip(d):
        def one(i, carry):
            v = av(0, 2 * ((x + d) % nx) + i)
            rms(v, v, 0)
            return carry

        lax.fori_loop(0, 2, one, 0)

    with jax.named_scope("norm_sh"):
        lax.fori_loop(0, nx, norm_shared, 0)
    wait(av(0, s), lsem)
    wait(U.at[pl.ds(0, 1), :, :, pl.ds(0, D)], ownsem.at[0])
    with jax.named_scope("norm_own"):
        norm_chip(0)

    def unit(n):
        m = n - q4
        odd = (n >= q4) & (m % 2 == 1)
        kk = jnp.where(odd, 1, 0)
        hg = jnp.where(odd, 2 * (m // 2) + c, jnp.where(n < q4, n, q4 + m // 2))
        return kk, hg

    def unit_row(kk, xx):
        return RC * ((xx + nx) % nx) + jnp.where(kk == 1, 2, c)

    def unit_load(n):
        kk, hg = unit(n)

        @pl.when(kk == 0)
        def _():
            with jax.named_scope("wd"):
                d_wait(HGc, hg)

        w_load(HGc, hg, n % 2)

    NFO = 3 * q4 - 1
    QT = 2 * NS * SUB
    PT = 8 * NS * SUB
    NQT = NRB // 2
    scale2 = (HEAD ** -0.5) * math.log2(math.e)

    def unit_proj(n):
        kk, hg = unit(n)
        slot = n % 2

        @pl.when(n == 2)
        def _():
            with jax.named_scope("wfa2"):
                wait(FA.at[2], fasem.at[2])
            rcopy(FA.at[2], av(1, 2 * ((x + nx - 1 + 2 * c) % nx) + c), fassem, asem.at[1], over)

        @pl.when(n == q4)
        def _():
            with jax.named_scope("wsh"):
                wait(U.at[pl.ds(0, nx - 1), :, :, pl.ds(0, D)], asem.at[1])
            for d in range(1, nx):
                src = 2 * ((x + d) % nx) + c
                rcopy(av(1, src), av(1, src), shsem, asem.at[2], sib)

        @pl.when(n == q4 + 1)
        def _():
            wait(U.at[pl.ds(0, NRB // 2), :, :, pl.ds(0, D)], asem.at[2])

        with jax.named_scope("ww"):
            w_wait(HGc, slot)

        def proj(t, cr):
            rows = pl.ds(pl.multiple_of(t * PT, PT), PT)
            a = U[pl.ds(t * 8, 8), :, :, pl.ds(pl.multiple_of(kk * D, 128), D)].reshape(PT, D)
            cs = cos_t[rows, :]
            sn = sin_t[rows, :]
            for wi, dst in enumerate((QS, KS)):
                p = jnp.dot(a, W[slot, pl.ds(wi * D, D), :], preferred_element_type=F32)
                for h in range(CB // HEAD):
                    ph = p[:, h * HEAD:(h + 1) * HEAD]
                    dst[rows, h * HEAD:(h + 1) * HEAD] = (ph * cs + pltpu.roll(ph, HEAD // 2, 1) * sn).astype(BF16)
            VS[rows, :] = jnp.dot(a, W[slot, pl.ds(2 * D, D), :], preferred_element_type=F32).astype(BF16)
            return cr

        with jax.named_scope("proj"):
            lax.fori_loop(0, NRB // 8, proj, 0)

    def unit_attn(n):
        kk, hg = unit(n)
        hcols = pl.ds(pl.multiple_of(hg * CB, CB), CB)

        @pl.when((n >= q4) & (n + 1 < 3 * q4))
        def _():
            unit_load(n + 1)

        def head(h, cr):
            hc = pl.ds(pl.multiple_of(h * HEAD, HEAD), HEAD)
            for t in range(NQT):
                kl = (t + 1) * QT
                sc = lax.dot_general(QS[pl.ds(t * QT, QT), hc], KS[pl.ds(0, kl), hc], (((1,), (1,)), ((), ())), preferred_element_type=F32)
                diag = jnp.where(mask_t[...] > 0.0, sc[:, t * QT:], MASKED)
                if t:
                    sc = jnp.concatenate([sc[:, :t * QT], diag], axis=1)
                else:
                    sc = diag
                mx = jnp.max(sc, axis=-1, keepdims=True)
                p = jnp.exp2((sc - mx) * scale2)
                ls = jnp.sum(p, axis=-1, keepdims=True)
                o = jnp.dot(p.astype(BF16), VS[pl.ds(0, kl), hc], preferred_element_type=F32)
                o = (o * (1.0 / ls)).astype(BF16)
                OST[n, pl.ds(2 * t, 2), :, :, hc] = o.reshape(2, NS, SUB, HEAD)
            return cr

        with jax.named_scope("attn"):
            lax.fori_loop(0, CB // HEAD, head, 0)

        row = unit_row(kk, x)
        B[row, :, :, hcols] = OST[n, :, s]
        rcopy(OST.at[n, :, 2 * x + 1 - c], B.at[row, :, :, hcols], ossem.at[n], osem.at[row], sib)

        @pl.when(n < NFO)
        def _():
            rcopy(OST.at[n, :, pl.ds(2 * far, 2)], FO.at[n], ossem.at[n], fosem.at[n], over)

        @pl.when(n >= NFO)
        def _():
            for cc in range(2):
                rcopy(OST.at[n, :, 2 * far + cc], B.at[row, :, :, hcols], ossem.at[n], osem.at[row], dev(far, cc))

        for dx in (1, nx - 1):
            for cc in range(2):
                xd = (x + dx) % nx
                rcopy(OST.at[n, :, 2 * xd + cc], B.at[row, :, :, hcols], ossem.at[n], osem.at[row], dev(xd, cc))

        @pl.when(n < q4)
        def _():
            unit_load(n + 1)

    def unit_forward(n):
        kk, hg = unit(n)
        wait(FO.at[n], fosem.at[n])
        row = unit_row(kk, x - 1 + 2 * c)
        for cc in range(2):
            rcopy(FO.at[n, :, cc], B.at[row, :, :, pl.ds(pl.multiple_of(hg * CB, CB), CB)], fossem.at[n], osem.at[row], dev(x + 1 - 2 * c, cc))

    MT = ROWS // 2
    NMT = ROWS // MT
    TM = MT * NRB * SUB

    def xc_load(j, slot):
        return pltpu.make_async_copy(x_hbm.at[:, :, :, pl.ds(pl.multiple_of(j * CB, CB), CB)], XC.at[slot], xcsem.at[slot])

    def yc_copy(j, slot):
        return pltpu.make_async_copy(YC.at[slot], out.at[:, :, :, pl.ds(pl.multiple_of(j * CB, CB), CB)], ycsem.at[slot])

    def yc_part(j, slot, rr):
        return pltpu.make_async_copy(YC.at[slot, rr], out.at[rr, :, :, pl.ds(pl.multiple_of(j * CB, CB), CB)], ycsem.at[slot])

    def prep(qn):
        for k in (Oc, GUc, DNc):
            j = qn + HGc["n"] - k["base"]

            @pl.when((j >= 0) & (j < k["n"]))
            def _(k=k, j=j):
                with jax.named_scope("wd"):
                    d_wait(k, j)
                w_load(k, j, qn % 2)
                if k is Oc:
                    xc_load(j, qn % 2).start()

    def o_step(j):
        slot = j % 2
        w_wait(Oc, slot)
        xc_load(j, slot).wait()
        prep(j + 1)
        cols = pl.ds(pl.multiple_of(j * CB, CB), CB)

        def tile(t, cr):
            rr = pl.ds(t * MT, MT)
            p = jnp.dot(B[rr].reshape(TM, D), W[slot, pl.ds(0, D), :], preferred_element_type=F32)
            h = XC[slot, rr].reshape(TM, CB).astype(F32) + p
            H[rr, :, :, cols] = h.astype(BF16).reshape(MT, NRB, SUB, CB)
            return cr

        lax.fori_loop(0, NMT, tile, 0)

    def gu_part(j, t):
        qn = Oc["n"] + j
        slot = qn % 2

        @pl.when(t == 0)
        def _():
            w_wait(GUc, slot)
            prep(qn + 1)

        cols = pl.ds(col0(GUc, j), CB)
        rr = pl.ds(t * MT, MT)
        b = B[rr].reshape(TM, D)
        g = jnp.dot(b, W[slot, pl.ds(0, D), :], preferred_element_type=F32)
        u = jnp.dot(b, W[slot, pl.ds(D, D), :], preferred_element_type=F32)
        act = g * (1.0 / (1.0 + jnp.exp(-g)))
        U[rr, :, :, cols] = (act * u).astype(BF16).reshape(MT, NRB, SUB, CB)

    def dn_part(j, t):
        qn = Oc["n"] + GUc["n"] + j
        slot = qn % 2
        ys = j % 2

        @pl.when(t == 0)
        def _():
            w_wait(DNc, slot)
            prep(qn + 1)

            @pl.when(j >= 2)
            def _():
                yc_copy(j - 2, ys).wait()

        cols = pl.ds(pl.multiple_of(j * CB, CB), CB)
        rr = pl.ds(t * MT, MT)
        p = jnp.dot(U[rr].reshape(TM, F), W[slot, pl.ds(0, F), :], preferred_element_type=F32)
        h = H[rr, :, :, cols].reshape(TM, CB).astype(F32) + p
        YC[ys, rr] = h.astype(BF16).reshape(MT, NRB, SUB, CB)
        yc_part(j, ys, rr).start()

    U0 = NPRE
    G0 = U0 + 6 * q4
    O0 = G0 + NGAP
    N0 = O0 + Oc["n"]
    GU0 = N0 + 2
    DN0 = GU0 + 2 * GUc["n"]
    NP = DN0 + 2 * DNc["n"]
    p1, p2, p3, po = pump_lists(NSTEP, NHG, GUc["n"], DNc["n"], NFO, U0, G0, O0, N0, GU0, DN0)
    first_two = GUc["base"]

    def run(lo, n, f):
        def go(i, cr):
            f(i)
            return cr

        lax.fori_loop(lo, lo + n, go, 0)
        return lo + n

    def ev1(i):
        each(i, lambda k: k["look"], s1_send)
        each(i, lambda k: 0, s1_done)

    def step(p, carry):
        e1, e2, e3, eo = carry
        with jax.named_scope("w1"):
            e1 = run(e1, due(p, p1), ev1)
        with jax.named_scope("w2"):
            e2 = run(e2, due(p, p2), lambda i: each(i, lambda k: 0, s2_done))
        with jax.named_scope("w3"):
            e3 = run(e3, due(p, p3), lambda i: each(i, lambda k: 0, x_done))
        with jax.named_scope("wfo"):
            eo = run(eo, due(p, po), unit_forward)

        @pl.when(p < 2)
        def _():
            with jax.named_scope("wfa"):
                wait(FA.at[p], fasem.at[p])
            rcopy(FA.at[p], av(0, 2 * ((x + nx - 1 + 2 * c) % nx) + c), fassem, ownsem.at[2], dev(x + 1 - 2 * c, p))

        @pl.when(p == 1)
        def _():
            rcopy(H.at[2], FA.at[2], assem, fasem.at[2], over)
            for d in (1, nx - 1):
                rcopy(H.at[d], av(1, s), assem, asem.at[1], dev(x + d, c))
            rcopy(H.at[0], av(1, s), assem, asem.at[2], sib)

        @pl.when((p >= 2) & (p < NPRE))
        def _():
            d = jnp.where(p == 2, 1, jnp.where(p == 3, nx - 1, 2))
            with jax.named_scope("wown"):
                wait(U.at[pl.ds(0, 2), :, :, pl.ds(0, D)], ownsem.at[d])
            with jax.named_scope("norm"):
                norm_chip(d)

        @pl.when(p == NPRE - 1)
        def _():
            unit_load(0)

        m = p - U0

        @pl.when((m >= 0) & (p < G0) & (m % 2 == 0))
        def _():
            unit_proj(m // 2)

        @pl.when((m >= 0) & (p < G0) & (m % 2 == 1))
        def _():
            unit_attn(m // 2)

        @pl.when(p == G0)
        def _():
            wait(H.at[pl.ds(0, ROWS - 1)], assem)
            wait(FA, fassem)
            wait(U.at[pl.ds(0, nx - 1), :, :, pl.ds(0, D)], shsem)
            prep(0)

        @pl.when(p == O0 - 1)
        def _():
            def orow(r, cr):
                k = r % RC

                @pl.when((r // RC != x) | (k == 1 - c))
                def _():
                    wait(B.at[r], osem.at[r])

                @pl.when((r // RC == x) & (k == 2))
                def _():
                    wait(B.at[r, pl.ds(0, NRB // 2)], osem.at[r])

                return cr

            with jax.named_scope("wo"):
                lax.fori_loop(0, ROWS, orow, 0)

        @pl.when((p >= O0) & (p < N0))
        def _():
            with jax.named_scope("ostep"):
                o_step(p - O0)

        @pl.when((p >= N0) & (p < GU0))
        def _():
            def nrow(r, cr):
                rms(H.at[r], B.at[r], 1)
                return cr

            with jax.named_scope("norm2"):
                lax.fori_loop((p - N0) * MT, (p - N0 + 1) * MT, nrow, 0)

        @pl.when((p >= GU0) & (p < DN0))
        def _():
            with jax.named_scope("gu"):
                gu_part((p - GU0) // 2, (p - GU0) % 2)

        @pl.when(p >= DN0)
        def _():
            with jax.named_scope("dn"):
                dn_part((p - DN0) // 2, (p - DN0) % 2)

        return e1, e2, e3, eo

    lax.fori_loop(0, NP, step, (0, 0, first_two, 0))

    for j in (DNc["n"] - 2, DNc["n"] - 1):
        yc_copy(j, j % 2).wait()

    def drain(n, cr):
        wait(OST.at[n, :, pl.ds(0, NS - 1)], ossem.at[n])

        @pl.when(n < NFO)
        def _():
            wait(FO.at[n], fossem.at[n])

        return cr

    lax.fori_loop(0, 3 * q4, drain, 0)
    wait(G.at[:, pl.ds(0, (nf - 1) * RD)], gssem)
    for k in classes:
        b, nr = k["buf"], k["nr"]
        wait(b.at[:, :, pl.ds(0, 2), pl.ds(0, nr)], ssem.at[k["ci"], 0])
        wait(b.at[:, :, 1, pl.ds(0, nr)], ssem.at[k["ci"], 1])
        if k["two"]:
            wait(b.at[:, :, :, pl.ds(0, nr)], ssem.at[k["ci"], 2])
        wait(b.at[:, :, :, pl.ds(0, k["R"] // 2)], ssem.at[k["ci"], 3])


def local_layer(x, norm_attn, wq, wk, wv, wo, norm_mlp, wg, wu, wd, *, nf, ns):
    rows, tl, D = x.shape
    F = wg.shape[1]
    nx = ns // 2
    nrb = tl // SUB
    nhg = D // CB
    ngu = -(-F // CB)
    units = 3 * nhg // 2
    rd, rf = D // nf, F // nf
    tok = ns * tl

    idx = np.arange(tok, dtype=np.int32)
    blk, src, low = idx // (ns * SUB), idx % (ns * SUB) // SUB, idx % SUB
    pos = (blk * SUB + low) * ns + src
    inv_freq = np.exp(np.arange(HEAD // 2, dtype=np.float32) * np.float32(-2.0 * math.log(THETA) / HEAD))
    ang = (pos.astype(np.float32)[:, None] * inv_freq[None, :]).astype(np.float64)
    cs, sn = np.cos(ang).astype(np.float32), np.sin(ang).astype(np.float32)
    cos_t = jnp.asarray(np.concatenate([cs, cs], axis=1))
    sin_t = jnp.asarray(np.concatenate([-sn, sn], axis=1))
    qt = 2 * ns * SUB
    mask_t = jnp.asarray((pos[None, :qt] <= pos[:qt, None]).astype(np.float32))
    x4 = x.reshape(rows, nrb, SUB, D)

    nsteps = nhg * 3 + ngu
    dma = pltpu.SemaphoreType.DMA
    anyspec = pl.BlockSpec(memory_space=pl.ANY)
    vspec = pl.BlockSpec(memory_space=pltpu.VMEM)
    outs = [
        jax.ShapeDtypeStruct((rows, nrb, SUB, D), BF16),
        jax.ShapeDtypeStruct((nhg, 3, nf - 1, rd, CB), BF16),
        jax.ShapeDtypeStruct((nhg, 1, nf - 1, rd, CB), BF16),
        jax.ShapeDtypeStruct((ngu, 2, nf - 1, rd, CB), BF16),
        jax.ShapeDtypeStruct((nhg, 1, nf - 1, rf, CB), BF16),
    ]
    wrows = max(3 * D, F)
    res = pl.pallas_call(
        functools.partial(kernel, (nf, nx, D, F, rows, nrb, ns)),
        out_shape=outs,
        in_specs=[anyspec] + [vspec] * 5 + [anyspec] * 7,
        out_specs=[anyspec] * 5,
        scratch_shapes=[
            pltpu.VMEM((rows, nrb, SUB, D), BF16),
            pltpu.VMEM((rows, nrb, SUB, D), BF16),
            pltpu.VMEM((rows, nrb, SUB, F), BF16),
            pltpu.VMEM((units, nrb, ns, SUB, CB), BF16),
            pltpu.VMEM((tok, CB), BF16),
            pltpu.VMEM((tok, CB), BF16),
            pltpu.VMEM((tok, CB), BF16),
            pltpu.VMEM((2, wrows, CB), BF16),
            pltpu.VMEM((rows // nx, nrb, SUB, D), BF16),
            pltpu.VMEM((units, nrb, 2, SUB, CB), BF16),
            pltpu.VMEM((8, rd), F32),
            pltpu.VMEM((8, D), F32),
            pltpu.VMEM((2, rows, nrb, SUB, CB), BF16),
            pltpu.VMEM((2, rows, nrb, SUB, CB), BF16),
            pltpu.VMEM((2, nrb, SUB, D), BF16),
            dma((nsteps, 4)),
            dma((4, 4)),
            dma,
            dma,
            dma((3,)),
            dma((nx,)),
            dma,
            dma((rows // nx,)),
            dma,
            dma,
            dma((rows,)),
            dma((units,)),
            dma((units,)),
            dma((units,)),
            dma((2,)),
            dma((2,)),
            dma((2,)),
            dma((2,)),
            dma,
        ],
        compiler_params=pltpu.CompilerParams(collective_id=0, has_side_effects=True, vmem_limit_bytes=66 * 1000 * 1000),
        cost_estimate=pl.CostEstimate(flops=170_000_000_000, bytes_accessed=400_000_000, transcendentals=0),
        name="layer",
    )(x4, norm_attn[None], norm_mlp[None], cos_t, sin_t, mask_t, wq, wk, wv, wo, wg, wu, wd)
    return res[0].reshape(rows, tl, D)


def solution(mesh):
    row = P(("dp", "fsdp"), "sp", None)
    wspec = P("fsdp", None)
    gspec = P("fsdp")
    fn = functools.partial(local_layer, nf=mesh.shape["fsdp"], ns=mesh.shape["sp"])
    specs = (row, gspec, wspec, wspec, wspec, wspec, gspec, wspec, wspec, wspec)
    return jax.shard_map(fn, mesh=mesh, in_specs=specs, out_specs=row, check_vma=False)
```

```python
import functools
import math

import jax
import jax.numpy as jnp
import numpy as np
from jax import lax
from jax.experimental import pallas as pl
from jax.experimental.pallas import tpu as pltpu
from jax.sharding import PartitionSpec as P

HEAD = 128
EPS = 1e-5
THETA = 5e7
MASKED = -1e30
CB = 256
SUB = 16
MESH = pl.DeviceIdType.MESH
F32 = jnp.float32
BF16 = jnp.bfloat16

PUMP1 = [0, 0, 2, 2, 8, 10, 13, 14, 16, 19, 21, 22, 23, 25, 25, 27, 27, 29, 30, 31, 33, 38, 38, 39, 42, 44, 46, 48, 51, 51, 55, 55, 57, 61, 61, 62, 64, 68, 70, 73, 75, 77, 82, 83, 87, 88]
PUMP2 = [0, 3, 8, 10, 12, 16, 18, 21, 28, 29, 29, 29, 29, 29, 29, 29, 31, 34, 36, 38, 40, 41, 43, 45, 47, 49, 51, 53, 55, 57, 59, 61, 63, 64, 67, 67, 70, 73, 76, 79, 81, 83, 86, 88, 89, 92]
PUMP3 = [0, 2, 10, 13, 22, 22, 25, 29, 29, 29, 29, 29, 29, 30, 30, 31, 35, 40, 40, 42, 44, 48, 49, 49, 52, 54, 56, 57, 59, 61, 63, 65, 67, 72, 75, 75, 75, 77, 81, 85, 86, 88, 91, 92, 95, 97]
PUMPO = [15, 15, 15, 17, 19, 19, 21, 23, 24, 27, 28]
NPRE = 5
NGAP = 3


def due(i, counts):
    words = [sum(v << (4 * q) for q, v in enumerate(counts[w:w + 7])) for w in range(0, len(counts), 7)]
    w = jnp.int32(words[0])
    for q, v in enumerate(words[1:], 1):
        w = jnp.where(i // 7 == q, v, w)
    return lax.shift_right_logical(w, 4 * (i % 7)) % 16


def pump_lists(nstep, nhg, ngu, ndn, nfo, u0, g0, o0, n0, gu0, dn0):
    q4 = nhg // 2
    need = []
    for h in range(nhg):
        n = h if h < q4 else q4 + 2 * (h - q4) + 1
        need.append(u0 + 2 * min(n, 3 * q4 - 2) - 1)
    need += [g0] + [o0 + j for j in range(nhg - 1)]
    need += [n0 - 1] + [gu0 + 2 * j for j in range(ngu - 1)]
    need += [dn0 - 2] + [dn0 + 2 * j for j in range(ndn - 1)]
    two = 2 * nhg
    if (nstep, nhg) == (len(PUMP1), 8):
        p1, p2, p3, po = PUMP1, PUMP2, PUMP3, PUMPO
    else:
        p1 = [max(0, q - 3) for q in need]
        p2 = [max(0, q - 2) for q in need]
        p3 = p2[:two] + [max(0, q - 1) for q in need[two:]]
        po = [u0 + 2 * n + 3 for n in range(nfo)]
    for i in range(nstep):
        last = p3[i] if i >= two else p2[i]
        assert p1[i] <= p2[i] <= last <= need[i], (i, p1[i], p2[i], last, need[i])
    assert all(po[n] > u0 + 2 * n + 1 for n in range(nfo)) and po[-1] < o0
    return p1, p2, p3, po


def kernel(cfg, x_hbm, g1, g2, cos_t, sin_t, mask_t, wq, wk, wv, wo, wg, wu, wd, out, bq, bo, bg, bd, H, B, U, OST, QS, KS, VS, W, WD, FA, FO, GL, G, XC, YC, XN,
           rsem, ssem, gsem, gssem, asem, ownsem, assem, fasem, fassem, shsem, osem, ossem, fosem, fossem, wsem, xcsem, ycsem, xnsem, lsem):
    nf, nx, D, F, ROWS, NRB, NS = cfg
    RC = ROWS // nx
    NHG = D // CB
    q4 = NHG // 2
    y = lax.axis_index("fsdp")
    s = lax.axis_index("sp")
    x = s // 2
    c = s % 2
    par = x % 2

    def dev(xx, cc):
        return {"sp": 2 * ((xx + nx) % nx) + cc}

    def ydev(d):
        return {"fsdp": (y + d + nf) % nf}

    sib = {"sp": 2 * x + 1 - c}

    def rcopy(src, dst, ssem_, rsem_, to):
        pltpu.make_async_remote_copy(src_ref=src, dst_ref=dst, send_sem=ssem_, recv_sem=rsem_, device_id=to, device_id_type=MESH).start()

    def wait(view, sem):
        pltpu.make_async_copy(view, view, sem).wait()

    NGU = pl.cdiv(F, CB)
    RD, RF = D // nf, F // nf
    classes = []
    base = 0
    for ws, buf, R, n, two, look in (
        ((wq, wk, wv), bq, RD, NHG, False, 2),
        ((wo,), bo, RD, NHG, False, 3),
        ((wg, wu), bg, RD, NGU, True, 3),
        ((wd,), bd, RF, NHG, True, 2),
    ):
        nr = R // 4 if two else R // 2
        ra = ((nr // 8 + 1) // 2) * 8
        p0 = pl.multiple_of((2 * par + c) * nr if two else c * nr, 8)
        q0 = pl.multiple_of((2 * (1 - par) + c) * nr, 8) if two else None
        ncols = ws[0].shape[1]
        classes.append(dict(ws=ws, buf=buf, R=R, n=n, base=base, two=two, look=look, nr=nr, ra=ra, p0=p0, q0=q0, ncols=ncols, ci=len(classes)))
        base += n
    NSTEP = base
    HGc, Oc, GUc, DNc = classes

    def col0(k, j):
        return pl.multiple_of(jnp.minimum(j * CB, k["ncols"] - CB), 128)

    def each(i, look, lo, hi, f):
        for k in classes:
            d = k["look"] if look else 0
            first, last = k["base"] - d, k["base"] + k["n"] - d
            if hi <= first or lo >= last:
                continue
            j = i + d - k["base"]
            if first <= lo and hi <= last:
                f(k, j)
            else:

                @pl.when((j >= 0) & (j < k["n"]))
                def _(k=k, j=j):
                    f(k, j)

    def s1_send(k, j):
        rows = pl.ds(k["p0"], k["nr"])
        cols = pl.ds(col0(k, j), CB)
        for wi, w in enumerate(k["ws"]):
            src = w.at[rows, cols]
            rcopy(src, k["buf"].at[j, wi, 2, rows], ssem.at[k["ci"], 0], rsem.at[k["base"] + j, 0], ydev(1))
            rcopy(src, k["buf"].at[j, wi, 0, rows], ssem.at[k["ci"], 0], rsem.at[k["base"] + j, 0], ydev(-1))

    def s1_done(k, j):
        b, ra, nr = k["buf"], k["ra"], k["nr"]
        with jax.named_scope("w1"):
            wait(b.at[j, :, pl.ds(0, 2), pl.ds(k["p0"], nr)], rsem.at[k["base"] + j, 0])
        A = pl.ds(k["p0"], ra)
        Z = pl.ds(pl.multiple_of(k["p0"] + ra, 8), nr - ra)
        rcopy(b.at[j, :, 2, A], b.at[j, :, 1, A], ssem.at[k["ci"], 1], rsem.at[k["base"] + j, 1], ydev(1))
        rcopy(b.at[j, :, 0, Z], b.at[j, :, 1, Z], ssem.at[k["ci"], 1], rsem.at[k["base"] + j, 1], ydev(-1))

    def s2_done(k, j):
        b, ra, nr = k["buf"], k["ra"], k["nr"]
        with jax.named_scope("w2"):
            wait(b.at[j, :, 1, pl.ds(k["p0"], nr)], rsem.at[k["base"] + j, 1])
        rows = pl.ds(k["p0"], nr)
        if k["two"]:
            A = pl.ds(k["p0"], ra)
            Z = pl.ds(pl.multiple_of(k["p0"] + ra, 8), nr - ra)
            rcopy(b.at[j, :, :, A], b.at[j, :, :, A], ssem.at[k["ci"], 2], rsem.at[k["base"] + j, 2], dev(x + 1, c))
            rcopy(b.at[j, :, :, Z], b.at[j, :, :, Z], ssem.at[k["ci"], 2], rsem.at[k["base"] + j, 2], dev(x - 1, c))
        rcopy(b.at[j, :, :, rows], b.at[j, :, :, rows], ssem.at[k["ci"], 3], rsem.at[k["base"] + j, 3], sib)

    def x_done(k, j):
        if k["two"]:
            b = k["buf"]
            rows = pl.ds(k["q0"], k["nr"])
            with jax.named_scope("w3"):
                wait(b.at[j, :, :, rows], rsem.at[k["base"] + j, 2])
            rcopy(b.at[j, :, :, rows], b.at[j, :, :, rows], ssem.at[k["ci"], 3], rsem.at[k["base"] + j, 3], sib)

    def d_wait(k, j):
        wait(k["buf"].at[j, :, :, pl.ds(0, k["R"] // 2)], rsem.at[k["base"] + j, 3])

    def w_load(k, j, slot):
        R = k["R"]
        cols = pl.ds(col0(k, j), CB)
        if R == RD:
            nw = len(k["ws"])
            for wi, w in enumerate(k["ws"]):
                pltpu.make_async_copy(w.at[:, cols], W.at[slot, wi, 0], wsem.at[slot]).start()
            pltpu.make_async_copy(k["buf"].at[j], W.at[slot, pl.ds(0, nw), pl.ds(1, nf - 1)], wsem.at[slot]).start()
        else:
            pltpu.make_async_copy(k["ws"][0].at[:, cols], WD.at[slot, pl.ds(pl.multiple_of(y * R, 8), R)], wsem.at[slot]).start()
            for r in range(1, nf):
                yy = (y + r) % nf
                pltpu.make_async_copy(k["buf"].at[j, 0, r - 1], WD.at[slot, pl.ds(pl.multiple_of(yy * R, 8), R)], wsem.at[slot]).start()

    def w_wait(k, slot):
        if k["R"] == RD:
            wait(W.at[slot, pl.ds(0, len(k["ws"]))], wsem.at[slot])
        else:
            wait(WD.at[slot], wsem.at[slot])

    def wmat(slot, wi):
        return W[slot, wi].reshape(D, CB)

    GL[...] = jnp.zeros_like(GL)
    GL[0:1, :] = g1[...].astype(F32).reshape(1, RD)
    GL[1:2, :] = g2[...].astype(F32).reshape(1, RD)
    bar = pltpu.get_barrier_semaphore()
    peers = [ydev(d) for d in range(1, nf)] + [dev(x + d, cc) for d in range(1, nx) for cc in range(2)] + [sib]
    for p in peers:
        pl.semaphore_signal(bar, inc=1, device_id=p, device_id_type=MESH)

    def av(k, src):
        return U.at[pl.ds(0, NRB), src, :, pl.ds(pl.multiple_of(k * D, 128), D)]

    def xn_load(i):
        r = RC * ((x + i) % nx) + 2
        return pltpu.make_async_copy(x_hbm.at[r], XN.at[i % 2], xnsem.at[i % 2])

    xn_load(0).start()
    pltpu.make_async_copy(x_hbm.at[RC * x + c], av(0, s), lsem).start()
    with jax.named_scope("bar"):
        pl.semaphore_wait(bar, len(peers))

    for d in range(1, nf):
        rcopy(GL, G.at[:, pl.ds((nf - d) * RD, RD)], gssem, gsem, ydev(d))
    for i in range(HGc["look"]):
        s1_send(HGc, i)
    over = dev(x + 1 - 2 * c, c)
    far = (x + 2) % nx
    rcopy(x_hbm.at[RC * x + 1 - c], av(0, s), assem, ownsem.at[0], sib)
    for k in range(2):
        rcopy(x_hbm.at[RC * far + k], FA.at[k], assem, fasem.at[k], over)
    for k in range(2):
        for d in (1, nx - 1):
            rcopy(x_hbm.at[RC * ((x + d) % nx) + k], av(0, s), assem, ownsem.at[nx - d], dev(x + d, k))
    G[:, 0:RD] = GL[...]
    with jax.named_scope("wg"):
        wait(G.at[:, pl.ds(0, (nf - 1) * RD)], gsem)

    turn = [pl.ds(pl.multiple_of((y + r) % nf * RD, 128), RD) for r in range(nf)]

    def rms(src, dst, grow):
        gs = [G[grow:grow + 1, r * RD:(r + 1) * RD] for r in range(nf)]

        def one(i, carry):
            hs = [src[i, :, t].astype(F32) for t in turn]
            sq = functools.reduce(lambda u, v: u + v, [h * h for h in hs])
            inv = lax.rsqrt(jnp.sum(sq, axis=-1, keepdims=True) * (1.0 / D) + EPS)
            for r in range(nf):
                dst[i, :, r * RD:(r + 1) * RD] = (hs[r] * inv * gs[r]).astype(BF16)
            return carry

        lax.fori_loop(0, NRB, one, 0, unroll=4)

    def norm_shared(i, carry):
        xn_load(i).wait()

        @pl.when(i + 1 < nx)
        def _():
            xn_load(i + 1).start()

        rms(XN.at[i % 2], H.at[i], 0)

        @pl.when(i == 0)
        def _():
            U[pl.ds(0, NRB), s, :, pl.ds(D, D)] = H[0]

        return carry

    def norm_chip(d):
        def one(i, carry):
            v = av(0, 2 * ((x + d) % nx) + i)
            rms(v, v, 0)
            return carry

        lax.fori_loop(0, 2, one, 0)

    with jax.named_scope("norm_sh"):
        lax.fori_loop(0, nx, norm_shared, 0)
    wait(av(0, s), lsem)
    wait(U.at[pl.ds(0, 1), :, :, pl.ds(0, D)], ownsem.at[0])
    with jax.named_scope("norm_own"):
        norm_chip(0)

    def unit(n):
        m = n - q4
        odd = (n >= q4) & (m % 2 == 0)
        kk = jnp.where(odd, 1, 0)
        hg = jnp.where(odd, 2 * (m // 2) + c, jnp.where(n < q4, n, q4 + m // 2))
        return kk, hg

    def turned(hg):
        return pl.ds(pl.multiple_of((hg * CB + D - y * RD) % D, CB), CB)

    def unit_row(kk, xx):
        return RC * ((xx + nx) % nx) + jnp.where(kk == 1, 2, c)

    def unit_load(n):
        kk, hg = unit(n)

        late = (c == 1) & (hg == NHG - 1)

        @pl.when(((kk == 0) & jnp.logical_not(late)) | ((kk == 1) & late))
        def _():
            with jax.named_scope("wd"):
                d_wait(HGc, hg)

        w_load(HGc, hg, n % 2)

    NFO = 3 * q4 - 1
    QT = 2 * NS * SUB
    PT = 8 * NS * SUB
    NQT = NRB // 2
    scale2 = (HEAD ** -0.5) * math.log2(math.e)

    def unit_proj(n):
        kk, hg = unit(n)
        slot = n % 2

        @pl.when(n == q4 - 2)
        def _():
            with jax.named_scope("wfa2"):
                wait(FA.at[2], fasem.at[2])
            rcopy(FA.at[2], av(1, 2 * ((x + nx - 1 + 2 * c) % nx) + c), fassem, asem.at[1], over)

        @pl.when(n == q4 - 1)
        def _():
            with jax.named_scope("wsh"):
                wait(U.at[pl.ds(0, nx - 1), :, :, pl.ds(0, D)], asem.at[1])
            for d in range(1, nx):
                src = 2 * ((x + d) % nx) + c
                rcopy(av(1, src), av(1, src), shsem, asem.at[2], sib)

        @pl.when(n == q4)
        def _():
            wait(U.at[pl.ds(0, NRB // 2), :, :, pl.ds(0, D)], asem.at[2])

        with jax.named_scope("ww"):
            w_wait(HGc, slot)

        def proj(t, cr):
            rows = pl.ds(pl.multiple_of(t * PT, PT), PT)
            a = U[pl.ds(t * 8, 8), :, :, pl.ds(pl.multiple_of(kk * D, 128), D)].reshape(PT, D)
            cs = cos_t[rows, :]
            sn = sin_t[rows, :]
            for wi, dst in enumerate((QS, KS)):
                p = jnp.dot(a, wmat(slot, wi), preferred_element_type=F32)
                for h in range(CB // HEAD):
                    ph = p[:, h * HEAD:(h + 1) * HEAD]
                    dst[rows, h * HEAD:(h + 1) * HEAD] = (ph * cs + pltpu.roll(ph, HEAD // 2, 1) * sn).astype(BF16)
            VS[rows, :] = jnp.dot(a, wmat(slot, 2), preferred_element_type=F32).astype(BF16)
            return cr

        with jax.named_scope("proj"):
            lax.fori_loop(0, NRB // 8, proj, 0)

    def unit_attn(n):
        kk, hg = unit(n)
        hcols = turned(hg)

        @pl.when((n >= q4 - 1) & (n + 1 < 3 * q4))
        def _():
            unit_load(n + 1)

        def scores(h, t):
            hc = pl.ds(h * HEAD, HEAD)
            qq = QS[pl.ds(t * QT, QT), hc]
            parts = []
            mp = None
            for kb in range(t + 1):
                sc = lax.dot_general(qq, KS[pl.ds(kb * QT, QT), hc], (((1,), (1,)), ((), ())), preferred_element_type=F32)
                if kb == t:
                    sc = jnp.where(mask_t[...] > 0.0, sc, MASKED)
                parts.append(sc)
                bm = jnp.maximum(sc[:, :HEAD], sc[:, HEAD:])
                mp = bm if mp is None else jnp.maximum(mp, bm)
            return parts, jnp.max(mp, axis=-1, keepdims=True) * scale2

        def mixed(h, t, parts, mx):
            hc = pl.ds(h * HEAD, HEAD)
            lp = None
            acc = None
            ps = []
            for kb in range(t + 1):
                p = jnp.exp2(parts[kb] * scale2 - mx)
                bs = p[:, :HEAD] + p[:, HEAD:]
                lp = bs if lp is None else lp + bs
                ps.append(p.astype(BF16))
            pc = jnp.concatenate(ps, axis=1) if t else ps[0]
            acc = jnp.dot(pc, VS[pl.ds(0, (t + 1) * QT), hc], preferred_element_type=F32)
            ls = jnp.sum(lp, axis=-1, keepdims=True)
            o = (acc * (1.0 / ls)).astype(BF16)
            OST[n, pl.ds(2 * t, 2), :, :, hc] = o.reshape(2, NS, SUB, HEAD)

        def heads():
            work = [(h, t) for t in reversed(range(NQT)) for h in range(CB // HEAD)]
            pend = []
            for h, t in work:
                pend.append((h, t) + scores(h, t))
                if len(pend) > 1:
                    mixed(*pend.pop(0))
            for w in pend:
                mixed(*w)

        with jax.named_scope("attn"):
            heads()

        row = unit_row(kk, x)
        B[row, :, :, hcols] = OST[n, :, s]
        rcopy(OST.at[n, :, 2 * x + 1 - c], B.at[row, :, :, hcols], ossem.at[n], osem.at[row], sib)

        @pl.when(n < NFO)
        def _():
            rcopy(OST.at[n, :, pl.ds(2 * far, 2)], FO.at[n], ossem.at[n], fosem.at[n], over)

        @pl.when(n >= NFO)
        def _():
            for cc in range(2):
                rcopy(OST.at[n, :, 2 * far + cc], B.at[row, :, :, hcols], ossem.at[n], osem.at[row], dev(far, cc))

        for dx in (1, nx - 1):
            for cc in range(2):
                xd = (x + dx) % nx
                rcopy(OST.at[n, :, 2 * xd + cc], B.at[row, :, :, hcols], ossem.at[n], osem.at[row], dev(xd, cc))

        @pl.when(n < q4 - 1)
        def _():
            unit_load(n + 1)

    def unit_forward(n):
        kk, hg = unit(n)
        with jax.named_scope("wfo"):
            wait(FO.at[n], fosem.at[n])
        row = unit_row(kk, x - 1 + 2 * c)
        for cc in range(2):
            rcopy(FO.at[n, :, cc], B.at[row, :, :, turned(hg)], fossem.at[n], osem.at[row], dev(x + 1 - 2 * c, cc))

    MT = ROWS // 2
    NMT = ROWS // MT
    TM = MT * NRB * SUB

    def xc_load(j, slot):
        return pltpu.make_async_copy(x_hbm.at[:, :, :, pl.ds(pl.multiple_of(j * CB, CB), CB)], XC.at[slot], xcsem.at[slot])

    def yc_copy(j, slot):
        return pltpu.make_async_copy(YC.at[slot], out.at[:, :, :, pl.ds(pl.multiple_of(j * CB, CB), CB)], ycsem.at[slot])

    def yc_part(j, slot, rr):
        return pltpu.make_async_copy(YC.at[slot, rr], out.at[rr, :, :, pl.ds(pl.multiple_of(j * CB, CB), CB)], ycsem.at[slot])

    def prep(qn):
        for k in (Oc, GUc, DNc):
            j = qn + HGc["n"] - k["base"]

            @pl.when((j >= 0) & (j < k["n"]))
            def _(k=k, j=j):
                with jax.named_scope("wd"):
                    d_wait(k, j)
                w_load(k, j, qn % 2)
                if k is Oc:
                    xc_load(j, qn % 2).start()

    def o_step(j):
        slot = j % 2
        w_wait(Oc, slot)
        xc_load(j, slot).wait()
        prep(j + 1)
        cols = pl.ds(pl.multiple_of(j * CB, CB), CB)

        def tile(t, cr):
            rr = pl.ds(t * MT, MT)
            p = jnp.dot(B[rr].reshape(TM, D), wmat(slot, 0), preferred_element_type=F32)
            h = XC[slot, rr].reshape(TM, CB).astype(F32) + p
            H[rr, :, :, cols] = h.astype(BF16).reshape(MT, NRB, SUB, CB)
            return cr

        with jax.named_scope("ostep"):
            lax.fori_loop(0, NMT, tile, 0)

    def gu_part(j, t):
        qn = Oc["n"] + j
        slot = qn % 2

        @pl.when(t == 0)
        def _():
            w_wait(GUc, slot)
            prep(qn + 1)

        cols = pl.ds(col0(GUc, j), CB)
        rr = pl.ds(t * MT, MT)
        b = B[rr].reshape(TM, D)
        g = jnp.dot(b, wmat(slot, 0), preferred_element_type=F32)
        u = jnp.dot(b, wmat(slot, 1), preferred_element_type=F32)
        act = g * (1.0 / (1.0 + jnp.exp(-g)))
        U[rr, :, :, cols] = (act * u).astype(BF16).reshape(MT, NRB, SUB, CB)

    def dn_part(j, t):
        qn = Oc["n"] + GUc["n"] + j
        slot = qn % 2
        ys = j % 2

        @pl.when(t == 0)
        def _():
            w_wait(DNc, slot)
            prep(qn + 1)

            @pl.when(j >= 2)
            def _():
                yc_copy(j - 2, ys).wait()

        cols = pl.ds(pl.multiple_of(j * CB, CB), CB)
        rr = pl.ds(t * MT, MT)
        p = jnp.dot(U[rr].reshape(TM, F), WD[slot], preferred_element_type=F32)
        h = H[rr, :, :, cols].reshape(TM, CB).astype(F32) + p
        YC[ys, rr] = h.astype(BF16).reshape(MT, NRB, SUB, CB)
        yc_part(j, ys, rr).start()

    U0 = NPRE
    G0 = U0 + 6 * q4
    O0 = G0 + NGAP
    N0 = O0 + Oc["n"]
    GU0 = N0 + 2
    DN0 = GU0 + 2 * GUc["n"]
    NP = DN0 + 2 * DNc["n"]
    lists = pump_lists(NSTEP, NHG, GUc["n"], DNc["n"], NFO, U0, G0, O0, N0, GU0, DN0)

    def ev1(i, lo, hi):
        each(i, True, lo, hi, s1_send)
        each(i, False, lo, hi, s1_done)

    def ev2(i, lo, hi):
        each(i, False, lo, hi, s2_done)

    def ev3(i, lo, hi):
        lo = max(lo, GUc["base"])
        if hi > lo:
            each(i, False, lo, hi, x_done)

    def evo(i, lo, hi):
        unit_forward(i)

    def phase(lo, hi, piece):
        plan = []
        for ev, pumps in zip((ev1, ev2, ev3, evo), lists):
            a = sum(q < lo for q in pumps)
            z = sum(q < hi for q in pumps)
            if ev is ev3:
                a, z = max(a, GUc["base"]), max(z, GUc["base"])
            counts = [sum(q == p for q in pumps[a:]) for p in range(lo, hi)]
            if z > a:
                plan.append((ev, a, z, counts))

        def body(p, es):
            out = []
            for (ev, a, z, counts), e in zip(plan, es):
                if min(counts) == max(counts) == 1:
                    ev(e, a, z)
                    out.append(e + 1)
                    continue
                n = due(p - lo, counts)
                if max(counts) == 1:

                    @pl.when(n == 1)
                    def _(ev=ev, e=e, a=a, z=z):
                        ev(e, a, z)
                else:

                    def go(i, cr, ev=ev, a=a, z=z):
                        ev(i, a, z)
                        return cr

                    lax.fori_loop(e, e + n, go, 0)
                out.append(e + n)
            piece(p)
            return tuple(out)

        lax.fori_loop(lo, hi, body, tuple(a for _, a, _, _ in plan))

    def pre_piece(p):
        @pl.when(p < 2)
        def _():
            with jax.named_scope("wfa"):
                wait(FA.at[p], fasem.at[p])
            rcopy(FA.at[p], av(0, 2 * ((x + nx - 1 + 2 * c) % nx) + c), fassem, ownsem.at[2], dev(x + 1 - 2 * c, p))

        @pl.when(p == 1)
        def _():
            rcopy(H.at[2], FA.at[2], assem, fasem.at[2], over)
            for d in (1, nx - 1):
                rcopy(H.at[d], av(1, s), assem, asem.at[1], dev(x + d, c))
            rcopy(H.at[0], av(1, s), assem, asem.at[2], sib)

        @pl.when(p >= 2)
        def _():
            d = jnp.where(p == 2, 1, jnp.where(p == 3, nx - 1, 2))
            with jax.named_scope("wown"):
                wait(U.at[pl.ds(0, 2), :, :, pl.ds(0, D)], ownsem.at[d])
            with jax.named_scope("norm"):
                norm_chip(d)

        @pl.when(p == NPRE - 1)
        def _():
            unit_load(0)

    def unit_piece(p):
        m = p - U0

        @pl.when(m % 2 == 0)
        def _():
            unit_proj(m // 2)

        @pl.when(m % 2 == 1)
        def _():
            unit_attn(m // 2)

    def gap_piece(p):
        @pl.when(p == G0)
        def _():
            wait(H.at[pl.ds(0, ROWS - 1)], assem)
            wait(FA, fassem)
            wait(U.at[pl.ds(0, nx - 1), :, :, pl.ds(0, D)], shsem)
            prep(0)

        @pl.when(p == O0 - 1)
        def _():
            def orow(r, cr):
                k = r % RC

                @pl.when((r // RC != x) | (k == 1 - c))
                def _():
                    wait(B.at[r], osem.at[r])

                @pl.when((r // RC == x) & (k == 2))
                def _():
                    wait(B.at[r, pl.ds(0, NRB // 2)], osem.at[r])

                return cr

            with jax.named_scope("wo"):
                lax.fori_loop(0, ROWS, orow, 0)

    def norm_piece(p):
        def nrow(r, cr):
            rms(H.at[r], B.at[r], 1)
            return cr

        with jax.named_scope("norm2"):
            lax.fori_loop((p - N0) * MT, (p - N0 + 1) * MT, nrow, 0)

    def scoped(name, f, i):
        with jax.named_scope(name):
            f(i // 2, i % 2)

    phase(0, U0, pre_piece)
    phase(U0, G0, unit_piece)
    phase(G0, O0, gap_piece)
    phase(O0, N0, lambda p: o_step(p - O0))
    phase(N0, GU0, norm_piece)
    phase(GU0, DN0, lambda p: scoped("gu", gu_part, p - GU0))
    phase(DN0, NP, lambda p: scoped("dn", dn_part, p - DN0))

    for j in (DNc["n"] - 2, DNc["n"] - 1):
        yc_copy(j, j % 2).wait()

    def drain(n, cr):
        wait(OST.at[n, :, pl.ds(0, NS - 1)], ossem.at[n])

        @pl.when(n < NFO)
        def _():
            wait(FO.at[n], fossem.at[n])

        return cr

    lax.fori_loop(0, 3 * q4, drain, 0)
    wait(G.at[:, pl.ds(0, (nf - 1) * RD)], gssem)
    for k in classes:
        b, nr = k["buf"], k["nr"]
        wait(b.at[:, :, pl.ds(0, 2), pl.ds(0, nr)], ssem.at[k["ci"], 0])
        wait(b.at[:, :, 1, pl.ds(0, nr)], ssem.at[k["ci"], 1])
        if k["two"]:
            wait(b.at[:, :, :, pl.ds(0, nr)], ssem.at[k["ci"], 2])
        wait(b.at[:, :, :, pl.ds(0, k["R"] // 2)], ssem.at[k["ci"], 3])


def local_layer(x, norm_attn, wq, wk, wv, wo, norm_mlp, wg, wu, wd, *, nf, ns):
    rows, tl, D = x.shape
    F = wg.shape[1]
    nx = ns // 2
    nrb = tl // SUB
    nhg = D // CB
    ngu = -(-F // CB)
    units = 3 * nhg // 2
    rd, rf = D // nf, F // nf
    tok = ns * tl

    idx = np.arange(tok, dtype=np.int32)
    blk, src, low = idx // (ns * SUB), idx % (ns * SUB) // SUB, idx % SUB
    pos = (blk * SUB + low) * ns + src
    inv_freq = np.exp(np.arange(HEAD // 2, dtype=np.float32) * np.float32(-2.0 * math.log(THETA) / HEAD))
    ang = (pos.astype(np.float32)[:, None] * inv_freq[None, :]).astype(np.float64)
    cs, sn = np.cos(ang).astype(np.float32), np.sin(ang).astype(np.float32)
    cos_t = jnp.asarray(np.concatenate([cs, cs], axis=1))
    sin_t = jnp.asarray(np.concatenate([-sn, sn], axis=1))
    qt = 2 * ns * SUB
    mask_t = jnp.asarray((pos[None, :qt] <= pos[:qt, None]).astype(np.float32))
    x4 = x.reshape(rows, nrb, SUB, D)

    nsteps = nhg * 3 + ngu
    dma = pltpu.SemaphoreType.DMA
    anyspec = pl.BlockSpec(memory_space=pl.ANY)
    vspec = pl.BlockSpec(memory_space=pltpu.VMEM)
    outs = [
        jax.ShapeDtypeStruct((rows, nrb, SUB, D), BF16),
        jax.ShapeDtypeStruct((nhg, 3, nf - 1, rd, CB), BF16),
        jax.ShapeDtypeStruct((nhg, 1, nf - 1, rd, CB), BF16),
        jax.ShapeDtypeStruct((ngu, 2, nf - 1, rd, CB), BF16),
        jax.ShapeDtypeStruct((nhg, 1, nf - 1, rf, CB), BF16),
    ]
    res = pl.pallas_call(
        functools.partial(kernel, (nf, nx, D, F, rows, nrb, ns)),
        out_shape=outs,
        in_specs=[anyspec] + [vspec] * 5 + [anyspec] * 7,
        out_specs=[anyspec] * 5,
        scratch_shapes=[
            pltpu.VMEM((rows, nrb, SUB, D), BF16),
            pltpu.VMEM((rows, nrb, SUB, D), BF16),
            pltpu.VMEM((rows, nrb, SUB, F), BF16),
            pltpu.VMEM((units, nrb, ns, SUB, CB), BF16),
            pltpu.VMEM((tok, CB), BF16),
            pltpu.VMEM((tok, CB), BF16),
            pltpu.VMEM((tok, CB), BF16),
            pltpu.VMEM((2, 3, nf, rd, CB), BF16),
            pltpu.VMEM((2, F, CB), BF16),
            pltpu.VMEM((rows // nx, nrb, SUB, D), BF16),
            pltpu.VMEM((units, nrb, 2, SUB, CB), BF16),
            pltpu.VMEM((8, rd), F32),
            pltpu.VMEM((8, D), F32),
            pltpu.VMEM((2, rows, nrb, SUB, CB), BF16),
            pltpu.VMEM((2, rows, nrb, SUB, CB), BF16),
            pltpu.VMEM((2, nrb, SUB, D), BF16),
            dma((nsteps, 4)),
            dma((4, 4)),
            dma,
            dma,
            dma((3,)),
            dma((nx,)),
            dma,
            dma((rows // nx,)),
            dma,
            dma,
            dma((rows,)),
            dma((units,)),
            dma((units,)),
            dma((units,)),
            dma((2,)),
            dma((2,)),
            dma((2,)),
            dma((2,)),
            dma,
        ],
        compiler_params=pltpu.CompilerParams(collective_id=0, has_side_effects=True, vmem_limit_bytes=66 * 1000 * 1000),
        cost_estimate=pl.CostEstimate(flops=170_000_000_000, bytes_accessed=400_000_000, transcendentals=0),
        name="layer",
    )(x4, norm_attn, norm_mlp, cos_t, sin_t, mask_t, wq, wk, wv, wo, wg, wu, wd)
    return res[0].reshape(rows, tl, D)


def solution(mesh):
    row = P(("dp", "fsdp"), "sp", None)
    wspec = P("fsdp", None)
    gspec = P("fsdp")
    fn = functools.partial(local_layer, nf=mesh.shape["fsdp"], ns=mesh.shape["sp"])
    specs = (row, gspec, wspec, wspec, wspec, wspec, gspec, wspec, wspec, wspec)
    return jax.shard_map(fn, mesh=mesh, in_specs=specs, out_specs=row, check_vma=False)
```

```python
import functools
import math

import jax
import jax.numpy as jnp
import numpy as np
from jax import lax
from jax.experimental import pallas as pl
from jax.experimental.pallas import tpu as pltpu
from jax.sharding import PartitionSpec as P

HEAD = 128
EPS = 1e-5
THETA = 5e7
MASKED = -1e30
CB = 256
SUB = 16
MESH = pl.DeviceIdType.MESH
F32 = jnp.float32
BF16 = jnp.bfloat16

PUMP1 = [0, 1, 1, 2, 7, 10, 16, 18, 18, 21, 22, 25, 25, 27, 27, 31, 31, 31, 35, 36, 37, 40, 42, 43, 44, 46, 48, 50, 52, 54, 57, 58, 62, 64, 65, 66, 68, 69, 73, 75, 78, 80, 84, 85, 88, 90]
PUMP2 = [3, 3, 5, 8, 11, 15, 20, 23, 26, 29, 29, 29, 30, 30, 31, 31, 34, 36, 38, 39, 41, 43, 45, 47, 49, 51, 52, 55, 57, 58, 60, 63, 64, 67, 68, 70, 71, 73, 76, 79, 82, 84, 86, 88, 90, 93]
PUMP3 = [0, 7, 8, 11, 11, 15, 25, 25, 28, 28, 28, 29, 29, 30, 30, 30, 37, 40, 41, 43, 46, 47, 50, 50, 53, 55, 58, 60, 62, 65, 65, 68, 69, 72, 74, 75, 76, 79, 82, 84, 86, 88, 90, 92, 95, 97]
PUMPO = [12, 14, 16, 18, 20, 20, 24, 24, 25, 27, 28]
NPRE = 5
NGAP = 3


def due(i, counts):
    words = [sum(v << (4 * q) for q, v in enumerate(counts[w:w + 7])) for w in range(0, len(counts), 7)]
    w = jnp.int32(words[0])
    for q, v in enumerate(words[1:], 1):
        w = jnp.where(i // 7 == q, v, w)
    return lax.shift_right_logical(w, 4 * (i % 7)) % 16


def pump_lists(nstep, nhg, ngu, ndn, nfo, u0, g0, o0, n0, gu0, dn0):
    q4 = nhg // 2
    need = []
    for h in range(nhg):
        n = h if h < q4 else q4 + 2 * (h - q4) + 1
        need.append(u0 + 2 * min(n, 3 * q4 - 2) - 1)
    need += [g0] + [o0 + j for j in range(nhg - 1)]
    need += [n0 - 1] + [gu0 + 2 * j for j in range(ngu - 1)]
    need += [dn0 - 2] + [dn0 + 2 * j for j in range(ndn - 1)]
    two = 2 * nhg
    if (nstep, nhg) == (len(PUMP1), 8):
        p1, p2, p3, po = PUMP1, PUMP2, PUMP3, PUMPO
    else:
        p1 = [max(0, q - 3) for q in need]
        p2 = [max(0, q - 2) for q in need]
        p3 = p2[:two] + [max(0, q - 1) for q in need[two:]]
        po = [u0 + 2 * n + 3 for n in range(nfo)]
    for i in range(nstep):
        last = p3[i] if i >= two else p2[i]
        assert p1[i] <= p2[i] <= last <= need[i], (i, p1[i], p2[i], last, need[i])
    assert all(po[n] > u0 + 2 * n + 1 for n in range(nfo)) and po[-1] < o0
    return p1, p2, p3, po


def kernel(cfg, x_hbm, g1, g2, cos_t, sin_t, mask_t, wq, wk, wv, wo, wg, wu, wd, B, bq, bo, bg, bd, H, U, OST, QS, KS, VS, W, WD, FA, FO, GL, G, XC, XN,
           rsem, ssem, gsem, gssem, asem, ownsem, assem, fasem, fassem, shsem, osem, ossem, fosem, fossem, wsem, xcsem, xnsem, lsem):
    nf, nx, D, F, ROWS, NRB, NS = cfg
    RC = ROWS // nx
    NHG = D // CB
    q4 = NHG // 2
    y = lax.axis_index("fsdp")
    s = lax.axis_index("sp")
    x = s // 2
    c = s % 2
    par = x % 2

    def dev(xx, cc):
        return {"sp": 2 * ((xx + nx) % nx) + cc}

    def ydev(d):
        return {"fsdp": (y + d + nf) % nf}

    sib = {"sp": 2 * x + 1 - c}

    def rcopy(src, dst, ssem_, rsem_, to):
        pltpu.make_async_remote_copy(src_ref=src, dst_ref=dst, send_sem=ssem_, recv_sem=rsem_, device_id=to, device_id_type=MESH).start()

    def wait(view, sem):
        pltpu.make_async_copy(view, view, sem).wait()

    NGU = pl.cdiv(F, CB)
    RD, RF = D // nf, F // nf
    classes = []
    base = 0
    for ws, buf, R, n, two, look in (
        ((wq, wk, wv), bq, RD, NHG, False, 2),
        ((wo,), bo, RD, NHG, False, 3),
        ((wg, wu), bg, RD, NGU, True, 3),
        ((wd,), bd, RF, NHG, True, 2),
    ):
        nr = R // 4 if two else R // 2
        ra = ((nr // 8 + 1) // 2) * 8
        p0 = pl.multiple_of((2 * par + c) * nr if two else c * nr, 8)
        q0 = pl.multiple_of((2 * (1 - par) + c) * nr, 8) if two else None
        ncols = ws[0].shape[1]
        classes.append(dict(ws=ws, buf=buf, R=R, n=n, base=base, two=two, look=look, nr=nr, ra=ra, p0=p0, q0=q0, ncols=ncols, ci=len(classes)))
        base += n
    NSTEP = base
    HGc, Oc, GUc, DNc = classes

    def col0(k, j):
        return pl.multiple_of(jnp.minimum(j * CB, k["ncols"] - CB), 128)

    def each(i, look, lo, hi, f):
        for k in classes:
            d = k["look"] if look else 0
            first, last = k["base"] - d, k["base"] + k["n"] - d
            if hi <= first or lo >= last:
                continue
            j = i + d - k["base"]
            if first <= lo and hi <= last:
                f(k, j)
            else:

                @pl.when((j >= 0) & (j < k["n"]))
                def _(k=k, j=j):
                    f(k, j)

    def s1_send(k, j):
        rows = pl.ds(k["p0"], k["nr"])
        cols = pl.ds(col0(k, j), CB)
        for wi, w in enumerate(k["ws"]):
            src = w.at[rows, cols]
            rcopy(src, k["buf"].at[j, wi, 2, rows], ssem.at[k["ci"], 0], rsem.at[k["base"] + j, 0], ydev(1))
            rcopy(src, k["buf"].at[j, wi, 0, rows], ssem.at[k["ci"], 0], rsem.at[k["base"] + j, 0], ydev(-1))

    def s1_done(k, j):
        b, ra, nr = k["buf"], k["ra"], k["nr"]
        with jax.named_scope("w1"):
            wait(b.at[j, :, pl.ds(0, 2), pl.ds(k["p0"], nr)], rsem.at[k["base"] + j, 0])
        A = pl.ds(k["p0"], ra)
        Z = pl.ds(pl.multiple_of(k["p0"] + ra, 8), nr - ra)
        rcopy(b.at[j, :, 2, A], b.at[j, :, 1, A], ssem.at[k["ci"], 1], rsem.at[k["base"] + j, 1], ydev(1))
        rcopy(b.at[j, :, 0, Z], b.at[j, :, 1, Z], ssem.at[k["ci"], 1], rsem.at[k["base"] + j, 1], ydev(-1))

    def s2_done(k, j):
        b, ra, nr = k["buf"], k["ra"], k["nr"]
        with jax.named_scope("w2"):
            wait(b.at[j, :, 1, pl.ds(k["p0"], nr)], rsem.at[k["base"] + j, 1])
        rows = pl.ds(k["p0"], nr)
        if k["two"]:
            A = pl.ds(k["p0"], ra)
            Z = pl.ds(pl.multiple_of(k["p0"] + ra, 8), nr - ra)
            rcopy(b.at[j, :, :, A], b.at[j, :, :, A], ssem.at[k["ci"], 2], rsem.at[k["base"] + j, 2], dev(x + 1, c))
            rcopy(b.at[j, :, :, Z], b.at[j, :, :, Z], ssem.at[k["ci"], 2], rsem.at[k["base"] + j, 2], dev(x - 1, c))
        rcopy(b.at[j, :, :, rows], b.at[j, :, :, rows], ssem.at[k["ci"], 3], rsem.at[k["base"] + j, 3], sib)

    def x_done(k, j):
        if k["two"]:
            b = k["buf"]
            rows = pl.ds(k["q0"], k["nr"])
            with jax.named_scope("w3"):
                wait(b.at[j, :, :, rows], rsem.at[k["base"] + j, 2])
            rcopy(b.at[j, :, :, rows], b.at[j, :, :, rows], ssem.at[k["ci"], 3], rsem.at[k["base"] + j, 3], sib)

    def d_wait(k, j):
        wait(k["buf"].at[j, :, :, pl.ds(0, k["R"] // 2)], rsem.at[k["base"] + j, 3])

    def w_load(k, j, slot):
        R = k["R"]
        cols = pl.ds(col0(k, j), CB)
        if R == RD:
            nw = len(k["ws"])
            for wi, w in enumerate(k["ws"]):
                pltpu.make_async_copy(w.at[:, cols], W.at[slot, wi, 0], wsem.at[slot]).start()
            pltpu.make_async_copy(k["buf"].at[j], W.at[slot, pl.ds(0, nw), pl.ds(1, nf - 1)], wsem.at[slot]).start()
        else:
            pltpu.make_async_copy(k["ws"][0].at[:, cols], WD.at[slot, pl.ds(pl.multiple_of(y * R, 8), R)], wsem.at[slot]).start()
            for r in range(1, nf):
                yy = (y + r) % nf
                pltpu.make_async_copy(k["buf"].at[j, 0, r - 1], WD.at[slot, pl.ds(pl.multiple_of(yy * R, 8), R)], wsem.at[slot]).start()

    def w_wait(k, slot):
        if k["R"] == RD:
            wait(W.at[slot, pl.ds(0, len(k["ws"]))], wsem.at[slot])
        else:
            wait(WD.at[slot], wsem.at[slot])

    def wmat(slot, wi):
        return W[slot, wi].reshape(D, CB)

    GL[...] = jnp.zeros_like(GL)
    GL[0:1, :] = g1[...].astype(F32).reshape(1, RD)
    GL[1:2, :] = g2[...].astype(F32).reshape(1, RD)
    bar = pltpu.get_barrier_semaphore()
    peers = [ydev(d) for d in range(1, nf)] + [dev(x + d, cc) for d in range(1, nx) for cc in range(2)] + [sib]
    for p in peers:
        pl.semaphore_signal(bar, inc=1, device_id=p, device_id_type=MESH)

    def av(k, src):
        return U.at[pl.ds(0, NRB), src, :, pl.ds(pl.multiple_of(k * D, 128), D)]

    def xn_load(i):
        r = RC * ((x + i) % nx) + 2
        return pltpu.make_async_copy(x_hbm.at[r], XN.at[i % 2], xnsem.at[i % 2])

    xn_load(0).start()
    pltpu.make_async_copy(x_hbm.at[RC * x + c], av(0, s), lsem).start()
    with jax.named_scope("bar"):
        pl.semaphore_wait(bar, len(peers))

    for d in range(1, nf):
        rcopy(GL, G.at[:, pl.ds((nf - d) * RD, RD)], gssem, gsem, ydev(d))
    for i in range(HGc["look"]):
        s1_send(HGc, i)
    over = dev(x + 1 - 2 * c, c)
    far = (x + 2) % nx
    rcopy(x_hbm.at[RC * x + 1 - c], av(0, s), assem, ownsem.at[0], sib)
    for k in range(2):
        rcopy(x_hbm.at[RC * far + k], FA.at[k], assem, fasem.at[k], over)
    for k in range(2):
        for d in (1, nx - 1):
            rcopy(x_hbm.at[RC * ((x + d) % nx) + k], av(0, s), assem, ownsem.at[nx - d], dev(x + d, k))
    G[:, 0:RD] = GL[...]
    with jax.named_scope("wg"):
        wait(G.at[:, pl.ds(0, (nf - 1) * RD)], gsem)

    turn = [pl.ds(pl.multiple_of((y + r) % nf * RD, 128), RD) for r in range(nf)]

    def rms(src, dst, grow):
        gs = [G[grow:grow + 1, r * RD:(r + 1) * RD] for r in range(nf)]

        def one(i, carry):
            hs = [src[i, :, t].astype(F32) for t in turn]
            sq = functools.reduce(lambda u, v: u + v, [h * h for h in hs])
            inv = lax.rsqrt(jnp.sum(sq, axis=-1, keepdims=True) * (1.0 / D) + EPS)
            for r in range(nf):
                dst[i, :, r * RD:(r + 1) * RD] = (hs[r] * inv * gs[r]).astype(BF16)
            return carry

        lax.fori_loop(0, NRB, one, 0, unroll=4)

    def norm_shared(i, carry):
        xn_load(i).wait()

        @pl.when(i + 1 < nx)
        def _():
            xn_load(i + 1).start()

        rms(XN.at[i % 2], H.at[i], 0)

        @pl.when(i == 0)
        def _():
            U[pl.ds(0, NRB), s, :, pl.ds(D, D)] = H[0]

        return carry

    def norm_chip(d):
        def one(i, carry):
            v = av(0, 2 * ((x + d) % nx) + i)
            rms(v, v, 0)
            return carry

        lax.fori_loop(0, 2, one, 0)

    with jax.named_scope("norm_sh"):
        lax.fori_loop(0, nx, norm_shared, 0)
    wait(av(0, s), lsem)
    wait(U.at[pl.ds(0, 1), :, :, pl.ds(0, D)], ownsem.at[0])
    with jax.named_scope("norm_own"):
        norm_chip(0)

    def unit(n):
        m = n - q4
        odd = (n >= q4) & (m % 2 == 0)
        kk = jnp.where(odd, 1, 0)
        hg = jnp.where(odd, 2 * (m // 2) + c, jnp.where(n < q4, n, q4 + m // 2))
        return kk, hg

    def turned(hg):
        return pl.ds(pl.multiple_of((hg * CB + D - y * RD) % D, CB), CB)

    def unit_row(kk, xx):
        return RC * ((xx + nx) % nx) + jnp.where(kk == 1, 2, c)

    def unit_load(n):
        kk, hg = unit(n)

        late = (c == 1) & (hg == NHG - 1)

        @pl.when(((kk == 0) & jnp.logical_not(late)) | ((kk == 1) & late))
        def _():
            with jax.named_scope("wd"):
                d_wait(HGc, hg)

        w_load(HGc, hg, n % 2)

    NFO = 3 * q4 - 1
    QT = 2 * NS * SUB
    PT = 8 * NS * SUB
    NQT = NRB // 2
    scale2 = (HEAD ** -0.5) * math.log2(math.e)

    def unit_proj(n):
        kk, hg = unit(n)
        slot = n % 2

        @pl.when(n == max(q4 - 3, 0))
        def _():
            with jax.named_scope("wfa2"):
                wait(FA.at[2], fasem.at[2])
            rcopy(FA.at[2], av(1, 2 * ((x + nx - 1 + 2 * c) % nx) + c), fassem, asem.at[1], over)

        @pl.when(n == q4 - 1)
        def _():
            with jax.named_scope("wsh"):
                wait(U.at[pl.ds(0, nx - 1), :, :, pl.ds(0, D)], asem.at[1])
            for d in range(1, nx):
                src = 2 * ((x + d) % nx) + c
                rcopy(av(1, src), av(1, src), shsem, asem.at[2], sib)

        @pl.when(n == q4)
        def _():
            wait(U.at[pl.ds(0, NRB // 2), :, :, pl.ds(0, D)], asem.at[2])

        with jax.named_scope("ww"):
            w_wait(HGc, slot)

        def proj(t, cr):
            rows = pl.ds(pl.multiple_of(t * PT, PT), PT)
            a = U[pl.ds(t * 8, 8), :, :, pl.ds(pl.multiple_of(kk * D, 128), D)].reshape(PT, D)
            cs = cos_t[rows, :]
            sn = sin_t[rows, :]
            for wi, dst in enumerate((QS, KS)):
                p = jnp.dot(a, wmat(slot, wi), preferred_element_type=F32)
                for h in range(CB // HEAD):
                    ph = p[:, h * HEAD:(h + 1) * HEAD]
                    dst[rows, h * HEAD:(h + 1) * HEAD] = (ph * cs + pltpu.roll(ph, HEAD // 2, 1) * sn).astype(BF16)
            VS[rows, :] = jnp.dot(a, wmat(slot, 2), preferred_element_type=F32).astype(BF16)
            return cr

        with jax.named_scope("proj"):
            lax.fori_loop(0, NRB // 8, proj, 0)

    def unit_attn(n):
        kk, hg = unit(n)
        hcols = turned(hg)

        @pl.when(n + 1 < 3 * q4)
        def _():
            unit_load(n + 1)

        def scores(h, t):
            hc = pl.ds(h * HEAD, HEAD)
            qq = QS[pl.ds(t * QT, QT), hc]
            parts = []
            mp = None
            for kb in range(t + 1):
                sc = lax.dot_general(qq, KS[pl.ds(kb * QT, QT), hc], (((1,), (1,)), ((), ())), preferred_element_type=F32)
                if kb == t:
                    sc = jnp.where(mask_t[...] > 0.0, sc, MASKED)
                parts.append(sc)
                bm = jnp.maximum(sc[:, :HEAD], sc[:, HEAD:])
                mp = bm if mp is None else jnp.maximum(mp, bm)
            return parts, jnp.max(mp, axis=-1, keepdims=True) * scale2

        def mixed(h, t, parts, mx):
            hc = pl.ds(h * HEAD, HEAD)
            lp = None
            acc = None
            ps = []
            for kb in range(t + 1):
                p = jnp.exp2(parts[kb] * scale2 - mx)
                bs = p[:, :HEAD] + p[:, HEAD:]
                lp = bs if lp is None else lp + bs
                ps.append(p.astype(BF16))
            pc = jnp.concatenate(ps, axis=1) if t else ps[0]
            acc = jnp.dot(pc, VS[pl.ds(0, (t + 1) * QT), hc], preferred_element_type=F32)
            ls = jnp.sum(lp, axis=-1, keepdims=True)
            o = (acc * (1.0 / ls)).astype(BF16)
            OST[n, pl.ds(2 * t, 2), :, :, hc] = o.reshape(2, NS, SUB, HEAD)

        def heads():
            work = [(h, t) for t in reversed(range(NQT)) for h in range(CB // HEAD)]
            pend = []
            for h, t in work:
                pend.append((h, t) + scores(h, t))
                if len(pend) > 1:
                    mixed(*pend.pop(0))
            for w in pend:
                mixed(*w)

        with jax.named_scope("attn"):
            heads()

        row = unit_row(kk, x)
        B[row, :, :, hcols] = OST[n, :, s]
        rcopy(OST.at[n, :, 2 * x + 1 - c], B.at[row, :, :, hcols], ossem.at[n], osem.at[row], sib)

        @pl.when(n < NFO)
        def _():
            rcopy(OST.at[n, :, pl.ds(2 * far, 2)], FO.at[n], ossem.at[n], fosem.at[n], over)

        @pl.when(n >= NFO)
        def _():
            for cc in range(2):
                rcopy(OST.at[n, :, 2 * far + cc], B.at[row, :, :, hcols], ossem.at[n], osem.at[row], dev(far, cc))

        for dx in (1, nx - 1):
            for cc in range(2):
                xd = (x + dx) % nx
                rcopy(OST.at[n, :, 2 * xd + cc], B.at[row, :, :, hcols], ossem.at[n], osem.at[row], dev(xd, cc))

    def unit_forward(n):
        kk, hg = unit(n)
        with jax.named_scope("wfo"):
            wait(FO.at[n], fosem.at[n])
        row = unit_row(kk, x - 1 + 2 * c)
        for cc in range(2):
            rcopy(FO.at[n, :, cc], B.at[row, :, :, turned(hg)], fossem.at[n], osem.at[row], dev(x + 1 - 2 * c, cc))

    MT = ROWS // 2
    NMT = ROWS // MT
    TM = MT * NRB * SUB

    def xc_load(j, slot):
        return pltpu.make_async_copy(x_hbm.at[:, :, :, pl.ds(pl.multiple_of(j * CB, CB), CB)], XC.at[slot], xcsem.at[slot])

    def prep(qn):
        for k in (Oc, GUc, DNc):
            j = qn + HGc["n"] - k["base"]

            @pl.when((j >= 0) & (j < k["n"]))
            def _(k=k, j=j):
                with jax.named_scope("wd"):
                    d_wait(k, j)
                w_load(k, j, qn % 2)
                if k is Oc:
                    xc_load(j, qn % 2).start()

    def o_step(j):
        slot = j % 2
        w_wait(Oc, slot)
        xc_load(j, slot).wait()
        prep(j + 1)
        cols = pl.ds(pl.multiple_of(j * CB, CB), CB)

        def tile(t, cr):
            rr = pl.ds(t * MT, MT)
            p = jnp.dot(B[rr].reshape(TM, D), wmat(slot, 0), preferred_element_type=F32)
            h = XC[slot, rr].reshape(TM, CB).astype(F32) + p
            H[rr, :, :, cols] = h.astype(BF16).reshape(MT, NRB, SUB, CB)
            return cr

        with jax.named_scope("ostep"):
            lax.fori_loop(0, NMT, tile, 0)

    def gu_part(j, t):
        qn = Oc["n"] + j
        slot = qn % 2

        @pl.when(t == 0)
        def _():
            w_wait(GUc, slot)
            prep(qn + 1)

        cols = pl.ds(col0(GUc, j), CB)
        rr = pl.ds(t * MT, MT)
        b = B[rr].reshape(TM, D)
        g = jnp.dot(b, wmat(slot, 0), preferred_element_type=F32)
        u = jnp.dot(b, wmat(slot, 1), preferred_element_type=F32)
        act = g * (1.0 / (1.0 + jnp.exp(-g)))
        U[rr, :, :, cols] = (act * u).astype(BF16).reshape(MT, NRB, SUB, CB)

    def dn_part(j, t):
        qn = Oc["n"] + GUc["n"] + j
        slot = qn % 2

        @pl.when(t == 0)
        def _():
            w_wait(DNc, slot)
            prep(qn + 1)

        cols = pl.ds(pl.multiple_of(j * CB, CB), CB)
        rr = pl.ds(t * MT, MT)
        p = jnp.dot(U[rr].reshape(TM, F), WD[slot], preferred_element_type=F32)
        h = H[rr, :, :, cols].reshape(TM, CB).astype(F32) + p
        B[rr, :, :, cols] = h.astype(BF16).reshape(MT, NRB, SUB, CB)

    U0 = NPRE
    G0 = U0 + 6 * q4
    O0 = G0 + NGAP
    N0 = O0 + Oc["n"]
    GU0 = N0 + 2
    DN0 = GU0 + 2 * GUc["n"]
    NP = DN0 + 2 * DNc["n"]
    lists = pump_lists(NSTEP, NHG, GUc["n"], DNc["n"], NFO, U0, G0, O0, N0, GU0, DN0)

    def ev1(i, lo, hi):
        each(i, False, lo, hi, s1_done)
        each(i, True, lo, hi, s1_send)

    def ev2(i, lo, hi):
        each(i, False, lo, hi, s2_done)

    def ev3(i, lo, hi):
        lo = max(lo, GUc["base"])
        if hi > lo:
            each(i, False, lo, hi, x_done)

    def evo(i, lo, hi):
        unit_forward(i)

    def phase(lo, hi, piece):
        plan = []
        for ev, pumps in zip((ev1, ev2, ev3, evo), lists):
            a = sum(q < lo for q in pumps)
            z = sum(q < hi for q in pumps)
            if ev is ev3:
                a, z = max(a, GUc["base"]), max(z, GUc["base"])
            counts = [sum(q == p for q in pumps[a:]) for p in range(lo, hi)]
            if z > a:
                plan.append((ev, a, z, counts))

        def body(p, es):
            out = []
            for (ev, a, z, counts), e in zip(plan, es):
                if min(counts) == max(counts) == 1:
                    ev(e, a, z)
                    out.append(e + 1)
                    continue
                n = due(p - lo, counts)
                if max(counts) == 1:

                    @pl.when(n == 1)
                    def _(ev=ev, e=e, a=a, z=z):
                        ev(e, a, z)
                else:

                    def go(i, cr, ev=ev, a=a, z=z):
                        ev(i, a, z)
                        return cr

                    lax.fori_loop(e, e + n, go, 0)
                out.append(e + n)
            piece(p)
            return tuple(out)

        lax.fori_loop(lo, hi, body, tuple(a for _, a, _, _ in plan))

    def pre_piece(p):
        @pl.when(p < 2)
        def _():
            with jax.named_scope("wfa"):
                wait(FA.at[p], fasem.at[p])
            rcopy(FA.at[p], av(0, 2 * ((x + nx - 1 + 2 * c) % nx) + c), fassem, ownsem.at[2], dev(x + 1 - 2 * c, p))

        @pl.when(p == 1)
        def _():
            rcopy(H.at[2], FA.at[2], assem, fasem.at[2], over)
            for d in (1, nx - 1):
                rcopy(H.at[d], av(1, s), assem, asem.at[1], dev(x + d, c))
            rcopy(H.at[0], av(1, s), assem, asem.at[2], sib)

        @pl.when(p == NPRE - 1)
        def _():
            unit_load(0)

        @pl.when(p >= 2)
        def _():
            d = jnp.where(p == 2, 1, jnp.where(p == 3, nx - 1, 2))
            with jax.named_scope("wown"):
                wait(U.at[pl.ds(0, 2), :, :, pl.ds(0, D)], ownsem.at[d])
            with jax.named_scope("norm"):
                norm_chip(d)

    def unit_piece(p):
        m = p - U0

        @pl.when(m % 2 == 0)
        def _():
            unit_proj(m // 2)

        @pl.when(m % 2 == 1)
        def _():
            unit_attn(m // 2)

    def gap_piece(p):
        @pl.when(p == G0)
        def _():
            wait(H.at[pl.ds(0, ROWS - 1)], assem)
            wait(FA, fassem)
            wait(U.at[pl.ds(0, nx - 1), :, :, pl.ds(0, D)], shsem)
            prep(0)

        @pl.when(p == O0 - 1)
        def _():
            def orow(r, cr):
                k = r % RC

                @pl.when((r // RC != x) | (k == 1 - c))
                def _():
                    wait(B.at[r], osem.at[r])

                @pl.when((r // RC == x) & (k == 2))
                def _():
                    wait(B.at[r, pl.ds(0, NRB // 2)], osem.at[r])

                return cr

            with jax.named_scope("wo"):
                lax.fori_loop(0, ROWS, orow, 0)

    def norm_piece(p):
        def nrow(r, cr):
            rms(H.at[r], B.at[r], 1)
            return cr

        with jax.named_scope("norm2"):
            lax.fori_loop((p - N0) * MT, (p - N0 + 1) * MT, nrow, 0)

    def scoped(name, f, i):
        with jax.named_scope(name):
            f(i // 2, i % 2)

    phase(0, U0, pre_piece)
    phase(U0, G0, unit_piece)
    phase(G0, O0, gap_piece)
    phase(O0, N0, lambda p: o_step(p - O0))
    phase(N0, GU0, norm_piece)
    phase(GU0, DN0, lambda p: scoped("gu", gu_part, p - GU0))
    phase(DN0, NP, lambda p: scoped("dn", dn_part, p - DN0))

    def drain(n, cr):
        wait(OST.at[n, :, pl.ds(0, NS - 1)], ossem.at[n])

        @pl.when(n < NFO)
        def _():
            wait(FO.at[n], fossem.at[n])

        return cr

    lax.fori_loop(0, 3 * q4, drain, 0)
    wait(G.at[:, pl.ds(0, (nf - 1) * RD)], gssem)
    for k in classes:
        b, nr = k["buf"], k["nr"]
        wait(b.at[:, :, pl.ds(0, 2), pl.ds(0, nr)], ssem.at[k["ci"], 0])
        wait(b.at[:, :, 1, pl.ds(0, nr)], ssem.at[k["ci"], 1])
        if k["two"]:
            wait(b.at[:, :, :, pl.ds(0, nr)], ssem.at[k["ci"], 2])
        wait(b.at[:, :, :, pl.ds(0, k["R"] // 2)], ssem.at[k["ci"], 3])


def local_layer(x, norm_attn, wq, wk, wv, wo, norm_mlp, wg, wu, wd, *, nf, ns):
    rows, tl, D = x.shape
    F = wg.shape[1]
    nx = ns // 2
    nrb = tl // SUB
    nhg = D // CB
    ngu = -(-F // CB)
    units = 3 * nhg // 2
    rd, rf = D // nf, F // nf
    tok = ns * tl

    idx = np.arange(tok, dtype=np.int32)
    blk, src, low = idx // (ns * SUB), idx % (ns * SUB) // SUB, idx % SUB
    pos = (blk * SUB + low) * ns + src
    inv_freq = np.exp(np.arange(HEAD // 2, dtype=np.float32) * np.float32(-2.0 * math.log(THETA) / HEAD))
    ang = (pos.astype(np.float32)[:, None] * inv_freq[None, :]).astype(np.float64)
    cs, sn = np.cos(ang).astype(np.float32), np.sin(ang).astype(np.float32)
    cos_t = jnp.asarray(np.concatenate([cs, cs], axis=1))
    sin_t = jnp.asarray(np.concatenate([-sn, sn], axis=1))
    qt = 2 * ns * SUB
    mask_t = jnp.asarray((pos[None, :qt] <= pos[:qt, None]).astype(np.float32))
    x4 = x.reshape(rows, nrb, SUB, D)

    nsteps = nhg * 3 + ngu
    dma = pltpu.SemaphoreType.DMA
    anyspec = pl.BlockSpec(memory_space=pl.ANY)
    vspec = pl.BlockSpec(memory_space=pltpu.VMEM)
    outs = [
        pltpu.VMEM((rows, nrb, SUB, D), BF16),
        jax.ShapeDtypeStruct((nhg, 3, nf - 1, rd, CB), BF16),
        jax.ShapeDtypeStruct((nhg, 1, nf - 1, rd, CB), BF16),
        jax.ShapeDtypeStruct((ngu, 2, nf - 1, rd, CB), BF16),
        jax.ShapeDtypeStruct((nhg, 1, nf - 1, rf, CB), BF16),
    ]
    res = pl.pallas_call(
        functools.partial(kernel, (nf, nx, D, F, rows, nrb, ns)),
        out_shape=outs,
        in_specs=[anyspec] + [vspec] * 5 + [anyspec] * 7,
        out_specs=[vspec] + [anyspec] * 4,
        scratch_shapes=[
            pltpu.VMEM((rows, nrb, SUB, D), BF16),
            pltpu.VMEM((rows, nrb, SUB, F), BF16),
            pltpu.VMEM((units, nrb, ns, SUB, CB), BF16),
            pltpu.VMEM((tok, CB), BF16),
            pltpu.VMEM((tok, CB), BF16),
            pltpu.VMEM((tok, CB), BF16),
            pltpu.VMEM((2, 3, nf, rd, CB), BF16),
            pltpu.VMEM((2, F, CB), BF16),
            pltpu.VMEM((rows // nx, nrb, SUB, D), BF16),
            pltpu.VMEM((units, nrb, 2, SUB, CB), BF16),
            pltpu.VMEM((8, rd), F32),
            pltpu.VMEM((8, D), F32),
            pltpu.VMEM((2, rows, nrb, SUB, CB), BF16),
            pltpu.VMEM((2, nrb, SUB, D), BF16),
            dma((nsteps, 4)),
            dma((4, 4)),
            dma,
            dma,
            dma((3,)),
            dma((nx,)),
            dma,
            dma((rows // nx,)),
            dma,
            dma,
            dma((rows,)),
            dma((units,)),
            dma((units,)),
            dma((units,)),
            dma((2,)),
            dma((2,)),
            dma((2,)),
            dma,
        ],
        compiler_params=pltpu.CompilerParams(collective_id=0, has_side_effects=True, vmem_limit_bytes=58 * 1000 * 1000),
        cost_estimate=pl.CostEstimate(flops=170_000_000_000, bytes_accessed=400_000_000, transcendentals=0),
        name="layer",
    )(x4, norm_attn, norm_mlp, cos_t, sin_t, mask_t, wq, wk, wv, wo, wg, wu, wd)
    return res[0].reshape(rows, tl, D)


def solution(mesh):
    row = P(("dp", "fsdp"), "sp", None)
    wspec = P("fsdp", None)
    gspec = P("fsdp")
    fn = functools.partial(local_layer, nf=mesh.shape["fsdp"], ns=mesh.shape["sp"])
    specs = (row, gspec, wspec, wspec, wspec, wspec, gspec, wspec, wspec, wspec)
    return jax.shard_map(fn, mesh=mesh, in_specs=specs, out_specs=row, check_vma=False)
```

```python
import functools
import math

import jax
import jax.numpy as jnp
import numpy as np
from jax import lax
from jax.experimental import pallas as pl
from jax.experimental.pallas import tpu as pltpu
from jax.sharding import PartitionSpec as P

HEAD = 128
EPS = 1e-5
THETA = 5e7
MASKED = -1e30
CB = 256
SUB = 16
MESH = pl.DeviceIdType.MESH
F32 = jnp.float32
BF16 = jnp.bfloat16

PUMP1 = [0, 1, 3, 4, 8, 10, 14, 17, 19, 20, 22, 24, 26, 27, 28, 29, 29, 31, 32, 34, 38, 38, 40, 41, 44, 45, 49, 50, 51, 55, 56, 59, 61, 61, 64, 65, 67, 70, 72, 74, 77, 80, 83, 86, 88, 91]
PUMP2 = [2, 4, 8, 9, 11, 14, 19, 22, 27, 30, 30, 30, 30, 31, 33, 33, 33, 35, 37, 38, 40, 42, 43, 46, 48, 50, 52, 54, 56, 58, 60, 62, 63, 65, 68, 69, 72, 73, 76, 79, 81, 83, 86, 88, 91, 93]
PUMP3 = [4, 13, 24, 24, 29, 31, 33, 34, 36, 38, 38, 38, 38, 38, 38, 38, 38, 38, 42, 42, 45, 48, 50, 52, 52, 54, 58, 58, 60, 61, 65, 65, 67, 72, 73, 75, 77, 78, 81, 84, 86, 88, 90, 92, 95, 97]
PUMPO = [8, 17, 17, 20, 22, 23, 24, 24, 25, 28, 31]
NPRE = 5
NGAP = 3


def due(i, counts):
    words = [sum(v << (4 * q) for q, v in enumerate(counts[w:w + 7])) for w in range(0, len(counts), 7)]
    w = jnp.int32(words[0])
    for q, v in enumerate(words[1:], 1):
        w = jnp.where(i // 7 == q, v, w)
    return lax.shift_right_logical(w, 4 * (i % 7)) % 16


def pump_lists(nstep, nhg, ngu, ndn, nfo, u0, g0, o0, n0, gu0, dn0):
    q4 = nhg // 2
    need = []
    for h in range(nhg):
        n = h if h < q4 else q4 + 2 * (h - q4)
        need.append((2, 4)[h] if h < 2 else u0 + 2 * n - 1)
    need += [g0] + [o0 + j for j in range(nhg - 1)]
    need += [n0 - 1] + [gu0 + 2 * j for j in range(ngu - 1)]
    need += [dn0 - 2] + [dn0 + 2 * j for j in range(ndn - 1)]
    two = 2 * nhg
    if (nstep, nhg) == (len(PUMP1), 8):
        p1, p2, p3, po = PUMP1, PUMP2, PUMP3, PUMPO
    else:
        p1 = [max(0, q - 3) for q in need]
        p2 = [max(0, q - 2) for q in need]
        p3 = p2[:two] + [max(0, q - 1) for q in need[two:]]
        po = [u0 + 2 * n + 3 for n in range(nfo)]
    for i in range(nstep):
        last = p3[i] if i >= two else p2[i]
        assert p1[i] <= p2[i] <= last <= need[i], (i, p1[i], p2[i], last, need[i])
    assert all(po[n] > u0 + 2 * n + 1 for n in range(nfo)) and po[-1] < o0
    return p1, p2, p3, po


def kernel(cfg, x_hbm, g1, g2, cos_t, sin_t, mask_t, wq, wk, wv, wo, wg, wu, wd, B, bq, bo, bg, bd, H, U, OST, QS, KS, VS, W, WD, FA, FO, GL, G, XC, XN,
           rsem, ssem, gsem, gssem, asem, ownsem, assem, fasem, fassem, shsem, osem, ossem, fosem, fossem, wsem, xcsem, xnsem, lsem):
    nf, nx, D, F, ROWS, NRB, NS = cfg
    RC = ROWS // nx
    NHG = D // CB
    q4 = NHG // 2
    y = lax.axis_index("fsdp")
    s = lax.axis_index("sp")
    x = s // 2
    c = s % 2
    par = x % 2

    def dev(xx, cc):
        return {"sp": 2 * ((xx + nx) % nx) + cc}

    def ydev(d):
        return {"fsdp": (y + d + nf) % nf}

    sib = {"sp": 2 * x + 1 - c}

    def rcopy(src, dst, ssem_, rsem_, to):
        pltpu.make_async_remote_copy(src_ref=src, dst_ref=dst, send_sem=ssem_, recv_sem=rsem_, device_id=to, device_id_type=MESH).start()

    def wait(view, sem):
        pltpu.make_async_copy(view, view, sem).wait()

    NGU = pl.cdiv(F, CB)
    RD, RF = D // nf, F // nf
    classes = []
    base = 0
    for ws, buf, R, n, two, look in (
        ((wq, wk, wv), bq, RD, NHG, False, 2),
        ((wo,), bo, RD, NHG, False, 3),
        ((wg, wu), bg, RD, NGU, True, 3),
        ((wd,), bd, RF, NHG, True, 2),
    ):
        nr = R // 4 if two else R // 2
        ra = ((nr // 8 + 1) // 2) * 8
        p0 = pl.multiple_of((2 * par + c) * nr if two else c * nr, 8)
        q0 = pl.multiple_of((2 * (1 - par) + c) * nr, 8) if two else None
        ncols = ws[0].shape[1]
        classes.append(dict(ws=ws, buf=buf, R=R, n=n, base=base, two=two, look=look, nr=nr, ra=ra, p0=p0, q0=q0, ncols=ncols, ci=len(classes)))
        base += n
    NSTEP = base
    HGc, Oc, GUc, DNc = classes

    def col0(k, j):
        return pl.multiple_of(jnp.minimum(j * CB, k["ncols"] - CB), 128)

    def each(i, look, lo, hi, f):
        for k in classes:
            d = k["look"] if look else 0
            first, last = k["base"] - d, k["base"] + k["n"] - d
            if hi <= first or lo >= last:
                continue
            j = i + d - k["base"]
            if first <= lo and hi <= last:
                f(k, j)
            else:

                @pl.when((j >= 0) & (j < k["n"]))
                def _(k=k, j=j):
                    f(k, j)

    def s1_send(k, j):
        rows = pl.ds(k["p0"], k["nr"])
        cols = pl.ds(col0(k, j), CB)
        for wi, w in enumerate(k["ws"]):
            src = w.at[rows, cols]
            rcopy(src, k["buf"].at[j, wi, 2, rows], ssem.at[k["ci"], 0], rsem.at[k["base"] + j, 0], ydev(1))
            rcopy(src, k["buf"].at[j, wi, 0, rows], ssem.at[k["ci"], 0], rsem.at[k["base"] + j, 0], ydev(-1))

    def s1_done(k, j):
        b, ra, nr = k["buf"], k["ra"], k["nr"]
        with jax.named_scope("w1"):
            wait(b.at[j, :, pl.ds(0, 2), pl.ds(k["p0"], nr)], rsem.at[k["base"] + j, 0])
        A = pl.ds(k["p0"], ra)
        Z = pl.ds(pl.multiple_of(k["p0"] + ra, 8), nr - ra)
        rcopy(b.at[j, :, 2, A], b.at[j, :, 1, A], ssem.at[k["ci"], 1], rsem.at[k["base"] + j, 1], ydev(1))
        rcopy(b.at[j, :, 0, Z], b.at[j, :, 1, Z], ssem.at[k["ci"], 1], rsem.at[k["base"] + j, 1], ydev(-1))

    def s2_done(k, j):
        b, ra, nr = k["buf"], k["ra"], k["nr"]
        with jax.named_scope("w2"):
            wait(b.at[j, :, 1, pl.ds(k["p0"], nr)], rsem.at[k["base"] + j, 1])
        rows = pl.ds(k["p0"], nr)
        if k["two"]:
            A = pl.ds(k["p0"], ra)
            Z = pl.ds(pl.multiple_of(k["p0"] + ra, 8), nr - ra)
            rcopy(b.at[j, :, :, A], b.at[j, :, :, A], ssem.at[k["ci"], 2], rsem.at[k["base"] + j, 2], dev(x + 1, c))
            rcopy(b.at[j, :, :, Z], b.at[j, :, :, Z], ssem.at[k["ci"], 2], rsem.at[k["base"] + j, 2], dev(x - 1, c))
        rcopy(b.at[j, :, :, rows], b.at[j, :, :, rows], ssem.at[k["ci"], 3], rsem.at[k["base"] + j, 3], sib)

    def x_done(k, j):
        if k["two"]:
            b = k["buf"]
            rows = pl.ds(k["q0"], k["nr"])
            with jax.named_scope("w3"):
                wait(b.at[j, :, :, rows], rsem.at[k["base"] + j, 2])
            rcopy(b.at[j, :, :, rows], b.at[j, :, :, rows], ssem.at[k["ci"], 3], rsem.at[k["base"] + j, 3], sib)

    def d_wait(k, j):
        wait(k["buf"].at[j, :, :, pl.ds(0, k["R"] // 2)], rsem.at[k["base"] + j, 3])

    def w_load(k, j, slot):
        R = k["R"]
        cols = pl.ds(col0(k, j), CB)
        if R == RD:
            nw = len(k["ws"])
            for wi, w in enumerate(k["ws"]):
                pltpu.make_async_copy(w.at[:, cols], W.at[slot, wi, 0], wsem.at[slot]).start()
            pltpu.make_async_copy(k["buf"].at[j], W.at[slot, pl.ds(0, nw), pl.ds(1, nf - 1)], wsem.at[slot]).start()
        else:
            pltpu.make_async_copy(k["ws"][0].at[:, cols], WD.at[slot, pl.ds(pl.multiple_of(y * R, 8), R)], wsem.at[slot]).start()
            for r in range(1, nf):
                yy = (y + r) % nf
                pltpu.make_async_copy(k["buf"].at[j, 0, r - 1], WD.at[slot, pl.ds(pl.multiple_of(yy * R, 8), R)], wsem.at[slot]).start()

    def w_wait(k, slot):
        if k["R"] == RD:
            wait(W.at[slot, pl.ds(0, len(k["ws"]))], wsem.at[slot])
        else:
            wait(WD.at[slot], wsem.at[slot])

    def wmat(slot, wi):
        return W[slot, wi].reshape(D, CB)

    GL[...] = jnp.zeros_like(GL)
    GL[0:1, :] = g1[...].astype(F32).reshape(1, RD)
    GL[1:2, :] = g2[...].astype(F32).reshape(1, RD)
    bar = pltpu.get_barrier_semaphore()
    peers = [ydev(d) for d in range(1, nf)] + [dev(x + d, cc) for d in range(1, nx) for cc in range(2)] + [sib]
    for p in peers:
        pl.semaphore_signal(bar, inc=1, device_id=p, device_id_type=MESH)

    def av(k, src):
        return U.at[pl.ds(0, NRB), src, :, pl.ds(pl.multiple_of(k * D, 128), D)]

    def xn_load(i):
        r = RC * ((x + i) % nx) + 2
        return pltpu.make_async_copy(x_hbm.at[r], XN.at[i % 2], xnsem.at[i % 2])

    xn_load(0).start()
    pltpu.make_async_copy(x_hbm.at[RC * x + c], av(0, s), lsem).start()
    with jax.named_scope("bar"):
        pl.semaphore_wait(bar, len(peers))

    for d in range(1, nf):
        rcopy(GL, G.at[:, pl.ds((nf - d) * RD, RD)], gssem, gsem, ydev(d))
    for i in range(HGc["look"]):
        s1_send(HGc, i)
    over = dev(x + 1 - 2 * c, c)
    far = (x + 2) % nx
    rcopy(x_hbm.at[RC * x + 1 - c], av(0, s), assem, ownsem.at[0], sib)
    for k in range(2):
        rcopy(x_hbm.at[RC * far + k], FA.at[k], assem, fasem.at[k], over)
    for k in range(2):
        for d in (1, nx - 1):
            rcopy(x_hbm.at[RC * ((x + d) % nx) + k], av(0, s), assem, ownsem.at[nx - d], dev(x + d, k))
    G[:, 0:RD] = GL[...]
    with jax.named_scope("wg"):
        wait(G.at[:, pl.ds(0, (nf - 1) * RD)], gsem)

    turn = [pl.ds(pl.multiple_of((y + r) % nf * RD, 128), RD) for r in range(nf)]

    def rms(src, dst, grow):
        gs = [G[grow:grow + 1, r * RD:(r + 1) * RD] for r in range(nf)]

        def some(i, carry):
            done = []
            for j in range(2):
                hs = [src[2 * i + j, :, t].astype(F32) for t in turn]
                sq = functools.reduce(lambda u, v: u + v, [h * h for h in hs])
                inv = lax.rsqrt(jnp.sum(sq, axis=-1, keepdims=True) * (1.0 / D) + EPS)
                done.append([(h * inv * g).astype(BF16) for h, g in zip(hs, gs)])
            for j in range(2):
                for r in range(nf):
                    dst[2 * i + j, :, r * RD:(r + 1) * RD] = done[j][r]
            return carry

        lax.fori_loop(0, NRB // 2, some, 0, unroll=2)

    def norm_shared(i, carry):
        xn_load(i).wait()

        @pl.when(i + 1 < nx)
        def _():
            xn_load(i + 1).start()

        rms(XN.at[i % 2], H.at[i], 0)

        @pl.when(i == 0)
        def _():
            U[pl.ds(0, NRB), s, :, pl.ds(D, D)] = H[0]

        return carry

    def norm_chip(d):
        def one(i, carry):
            v = av(0, 2 * ((x + d) % nx) + i)
            rms(v, v, 0)
            return carry

        lax.fori_loop(0, 2, one, 0)

    with jax.named_scope("norm_sh"):
        lax.fori_loop(0, nx, norm_shared, 0)
    wait(av(0, s), lsem)
    wait(U.at[pl.ds(0, 1), :, :, pl.ds(0, D)], ownsem.at[0])
    with jax.named_scope("norm_own"):
        norm_chip(0)

    def unit(n):
        m = n - q4
        odd = (n >= q4) & (m % 2 == 1)
        kk = jnp.where(odd, 1, 0)
        hg = jnp.where(odd, 2 * (m // 2) + c, jnp.where(n < q4, n, q4 + m // 2))
        return kk, hg

    def turned(hg):
        return pl.ds(pl.multiple_of((hg * CB + D - y * RD) % D, CB), CB)

    def unit_row(kk, xx):
        return RC * ((xx + nx) % nx) + jnp.where(kk == 1, 2, c)

    def unit_load(n):
        kk, hg = unit(n)

        @pl.when(kk == 0)
        def _():
            with jax.named_scope("wd"):
                d_wait(HGc, hg)

        w_load(HGc, hg, n % 2)

    NFO = 3 * q4 - 1
    QT = 2 * NS * SUB
    PT = 8 * NS * SUB
    NQT = NRB // 2
    scale2 = (HEAD ** -0.5) * math.log2(math.e)

    def project(n, kk, srcs):
        slot = n % 2
        rows = NRB * srcs.size * SUB
        a = U[pl.ds(0, NRB), srcs, :, pl.ds(pl.multiple_of(kk * D, 128), D)].reshape(rows, D)
        cs = cos_t[:, srcs].reshape(rows, HEAD)
        sn = sin_t[:, srcs].reshape(rows, HEAD)
        for wi, dst in enumerate((QS, KS)):
            p = jnp.dot(a, wmat(slot, wi), preferred_element_type=F32)
            for h in range(CB // HEAD):
                ph = p[:, h * HEAD:(h + 1) * HEAD]
                r = (ph * cs + pltpu.roll(ph, HEAD // 2, 1) * sn).astype(BF16)
                dst[slot, :, srcs, :, h * HEAD:(h + 1) * HEAD] = r.reshape(NRB, srcs.size, SUB, HEAD)
        v = jnp.dot(a, wmat(slot, 2), preferred_element_type=F32).astype(BF16)
        VS[slot, :, srcs] = v.reshape(NRB, srcs.size, SUB, CB)

    def proj_chip(n, d):
        project(n, 0, pl.ds(2 * ((x + d) % nx), 2))

    def unit_proj(n):
        kk, hg = unit(n)

        @pl.when(n == q4 + 1)
        def _():
            wait(U.at[pl.ds(0, NRB // 2), :, :, pl.ds(0, D)], asem.at[2])

        @pl.when(n < 2)
        def _():
            with jax.named_scope("proj"):
                proj_chip(n, 2)

        @pl.when(n >= 2)
        def _():
            with jax.named_scope("ww"):
                w_wait(HGc, n % 2)
            with jax.named_scope("proj"):
                project(n, kk, pl.ds(0, NS))

    def unit_attn(n):
        kk, hg = unit(n)
        hcols = turned(hg)

        @pl.when(n == max(q4 - 3, 0))
        def _():
            with jax.named_scope("wfa2"):
                wait(FA.at[2], fasem.at[2])
            rcopy(FA.at[2], av(1, 2 * ((x + nx - 1 + 2 * c) % nx) + c), fassem, asem.at[1], over)

        @pl.when(n == q4 - 1)
        def _():
            with jax.named_scope("wsh"):
                wait(U.at[pl.ds(0, nx - 1), :, :, pl.ds(0, D)], asem.at[1])
            for d in range(1, nx):
                src = 2 * ((x + d) % nx) + c
                rcopy(av(1, src), av(1, src), shsem, asem.at[2], sib)

        @pl.when((n > 0) & (n + 1 < 3 * q4))
        def _():
            unit_load(n + 1)

        def scores(h, t):
            hc = pl.ds(h * HEAD, HEAD)
            qq = QS[n % 2, pl.ds(2 * t, 2), :, :, hc].reshape(QT, HEAD)
            parts = []
            mp = None
            for kb in range(t + 1):
                sc = lax.dot_general(qq, KS[n % 2, pl.ds(2 * kb, 2), :, :, hc].reshape(QT, HEAD), (((1,), (1,)), ((), ())), preferred_element_type=F32)
                if kb == t:
                    sc = jnp.where(mask_t[...] > 0.0, sc, MASKED)
                parts.append(sc)
                bm = jnp.maximum(sc[:, :HEAD], sc[:, HEAD:])
                mp = bm if mp is None else jnp.maximum(mp, bm)
            return parts, jnp.max(mp, axis=-1, keepdims=True) * scale2

        def mixed(h, t, parts, mx):
            hc = pl.ds(h * HEAD, HEAD)
            lp = None
            acc = None
            ps = []
            for kb in range(t + 1):
                p = jnp.exp2(parts[kb] * scale2 - mx)
                bs = p[:, :HEAD] + p[:, HEAD:]
                lp = bs if lp is None else lp + bs
                ps.append(p.astype(BF16))
            pc = jnp.concatenate(ps, axis=1) if t else ps[0]
            acc = jnp.dot(pc, VS[n % 2, pl.ds(0, 2 * t + 2), :, :, hc].reshape((t + 1) * QT, HEAD), preferred_element_type=F32)
            ls = jnp.sum(lp, axis=-1, keepdims=True)
            o = (acc * (1.0 / ls)).astype(BF16)
            OST[n, pl.ds(2 * t, 2), :, :, hc] = o.reshape(2, NS, SUB, HEAD)

        def heads():
            work = [(h, t) for t in reversed(range(NQT)) for h in range(CB // HEAD)]
            pend = []
            for h, t in work:
                pend.append((h, t) + scores(h, t))
                if len(pend) > 1:
                    mixed(*pend.pop(0))
            for w in pend:
                mixed(*w)

        with jax.named_scope("attn"):
            heads()

        row = unit_row(kk, x)
        B[row, :, :, hcols] = OST[n, :, s]
        rcopy(OST.at[n, :, 2 * x + 1 - c], B.at[row, :, :, hcols], ossem.at[n], osem.at[row], sib)

        @pl.when(n < NFO)
        def _():
            rcopy(OST.at[n, :, pl.ds(2 * far, 2)], FO.at[n], ossem.at[n], fosem.at[n], over)

        @pl.when(n >= NFO)
        def _():
            for cc in range(2):
                rcopy(OST.at[n, :, 2 * far + cc], B.at[row, :, :, hcols], ossem.at[n], osem.at[row], dev(far, cc))

        for dx in (1, nx - 1):
            for cc in range(2):
                xd = (x + dx) % nx
                rcopy(OST.at[n, :, 2 * xd + cc], B.at[row, :, :, hcols], ossem.at[n], osem.at[row], dev(xd, cc))

    def unit_forward(n):
        kk, hg = unit(n)
        with jax.named_scope("wfo"):
            wait(FO.at[n], fosem.at[n])
        row = unit_row(kk, x - 1 + 2 * c)
        for cc in range(2):
            rcopy(FO.at[n, :, cc], B.at[row, :, :, turned(hg)], fossem.at[n], osem.at[row], dev(x + 1 - 2 * c, cc))

    MT = ROWS // 2
    NMT = ROWS // MT
    TM = MT * NRB * SUB

    def xc_load(j, slot):
        return pltpu.make_async_copy(x_hbm.at[:, :, :, pl.ds(pl.multiple_of(j * CB, CB), CB)], XC.at[slot], xcsem.at[slot])

    def prep(qn):
        for k in (Oc, GUc, DNc):
            j = qn + HGc["n"] - k["base"]

            @pl.when((j >= 0) & (j < k["n"]))
            def _(k=k, j=j):
                with jax.named_scope("wd"):
                    d_wait(k, j)
                w_load(k, j, qn % 2)
                if k is Oc:
                    xc_load(j, qn % 2).start()

    def o_step(j):
        slot = j % 2
        w_wait(Oc, slot)
        xc_load(j, slot).wait()
        prep(j + 1)
        cols = pl.ds(pl.multiple_of(j * CB, CB), CB)

        def tile(t, cr):
            rr = pl.ds(t * MT, MT)
            p = jnp.dot(B[rr].reshape(TM, D), wmat(slot, 0), preferred_element_type=F32)
            h = XC[slot, rr].reshape(TM, CB).astype(F32) + p
            H[rr, :, :, cols] = h.astype(BF16).reshape(MT, NRB, SUB, CB)
            return cr

        with jax.named_scope("ostep"):
            lax.fori_loop(0, NMT, tile, 0)

    def gu_part(j, t):
        qn = Oc["n"] + j
        slot = qn % 2

        @pl.when(t == 0)
        def _():
            w_wait(GUc, slot)
            prep(qn + 1)

        cols = pl.ds(col0(GUc, j), CB)
        rr = pl.ds(t * MT, MT)
        b = B[rr].reshape(TM, D)
        g = jnp.dot(b, wmat(slot, 0), preferred_element_type=F32)
        u = jnp.dot(b, wmat(slot, 1), preferred_element_type=F32)
        act = g * (1.0 / (1.0 + jnp.exp(-g)))
        U[rr, :, :, cols] = (act * u).astype(BF16).reshape(MT, NRB, SUB, CB)

    def dn_part(j, t):
        qn = Oc["n"] + GUc["n"] + j
        slot = qn % 2

        @pl.when(t == 0)
        def _():
            w_wait(DNc, slot)
            prep(qn + 1)

        cols = pl.ds(pl.multiple_of(j * CB, CB), CB)
        rr = pl.ds(t * MT, MT)
        p = jnp.dot(U[rr].reshape(TM, F), WD[slot], preferred_element_type=F32)
        h = H[rr, :, :, cols].reshape(TM, CB).astype(F32) + p
        B[rr, :, :, cols] = h.astype(BF16).reshape(MT, NRB, SUB, CB)

    U0 = NPRE
    G0 = U0 + 6 * q4
    O0 = G0 + NGAP
    N0 = O0 + Oc["n"]
    GU0 = N0 + 2
    DN0 = GU0 + 2 * GUc["n"]
    NP = DN0 + 2 * DNc["n"]
    lists = pump_lists(NSTEP, NHG, GUc["n"], DNc["n"], NFO, U0, G0, O0, N0, GU0, DN0)

    def ev1(i, lo, hi):
        each(i, False, lo, hi, s1_done)
        each(i, True, lo, hi, s1_send)

    def ev2(i, lo, hi):
        each(i, False, lo, hi, s2_done)

    def ev3(i, lo, hi):
        lo = max(lo, GUc["base"])
        if hi > lo:
            each(i, False, lo, hi, x_done)

    def evo(i, lo, hi):
        unit_forward(i)

    def phase(lo, hi, piece):
        plan = []
        for ev, pumps in zip((ev1, ev2, ev3, evo), lists):
            a = sum(q < lo for q in pumps)
            z = sum(q < hi for q in pumps)
            if ev is ev3:
                a, z = max(a, GUc["base"]), max(z, GUc["base"])
            counts = [sum(q == p for q in pumps[a:]) for p in range(lo, hi)]
            if z > a:
                plan.append((ev, a, z, counts))

        def body(p, es):
            out = []
            for (ev, a, z, counts), e in zip(plan, es):
                if min(counts) == max(counts) == 1:
                    ev(e, a, z)
                    out.append(e + 1)
                    continue
                n = due(p - lo, counts)
                if max(counts) == 1:

                    @pl.when(n == 1)
                    def _(ev=ev, e=e, a=a, z=z):
                        ev(e, a, z)
                else:

                    def go(i, cr, ev=ev, a=a, z=z):
                        ev(i, a, z)
                        return cr

                    lax.fori_loop(e, e + n, go, 0)
                out.append(e + n)
            piece(p)
            return tuple(out)

        lax.fori_loop(lo, hi, body, tuple(a for _, a, _, _ in plan))

    def shared_send(d):
        rcopy(H.at[d], av(1, s), assem, asem.at[1], dev(x + d, c))

    def chips(n):
        def go(i, cr):
            proj_chip(n, jnp.where(i == 2, nx - 1, i))
            return cr

        with jax.named_scope("chips"):
            lax.fori_loop(0, 3, go, 0)

    def pre_piece(p):
        @pl.when(p < 2)
        def _():
            with jax.named_scope("wfa"):
                wait(FA.at[p], fasem.at[p])
            rcopy(FA.at[p], av(0, 2 * ((x + nx - 1 + 2 * c) % nx) + c), fassem, ownsem.at[2], dev(x + 1 - 2 * c, p))

        @pl.when(p == 1)
        def _():
            rcopy(H.at[2], FA.at[2], assem, fasem.at[2], over)
            shared_send(1 + (nx - 2) * c)
            rcopy(H.at[0], av(1, s), assem, asem.at[2], sib)

        @pl.when(p == NPRE - 1)
        def _():
            unit_load(1)
            w_wait(HGc, 1)
            chips(1)
            shared_send(nx - 1 - (nx - 2) * c)

        @pl.when(p >= 2)
        def _():
            d = jnp.where(p == 2, 1, jnp.where(p == 3, nx - 1, 2))
            with jax.named_scope("wown"):
                wait(U.at[pl.ds(0, 2), :, :, pl.ds(0, D)], ownsem.at[d])
            with jax.named_scope("norm"):
                norm_chip(d)

        @pl.when(p == 2)
        def _():
            unit_load(0)

        @pl.when(p == 3)
        def _():
            w_wait(HGc, 0)
            chips(0)

    def unit_piece(p):
        m = p - U0

        @pl.when(m % 2 == 0)
        def _():
            unit_proj(m // 2)

        @pl.when(m % 2 == 1)
        def _():
            unit_attn(m // 2)

    def gap_piece(p):
        @pl.when(p == G0)
        def _():
            wait(H.at[pl.ds(0, ROWS - 1)], assem)
            wait(FA, fassem)
            wait(U.at[pl.ds(0, nx - 1), :, :, pl.ds(0, D)], shsem)
            prep(0)

        @pl.when(p == O0 - 1)
        def _():
            def orow(r, cr):
                k = r % RC

                @pl.when((r // RC != x) | (k == 1 - c))
                def _():
                    wait(B.at[r], osem.at[r])

                @pl.when((r // RC == x) & (k == 2))
                def _():
                    wait(B.at[r, pl.ds(0, NRB // 2)], osem.at[r])

                return cr

            with jax.named_scope("wo"):
                lax.fori_loop(0, ROWS, orow, 0)

    def norm_piece(p):
        def nrow(r, cr):
            rms(H.at[r], B.at[r], 1)
            return cr

        with jax.named_scope("norm2"):
            lax.fori_loop((p - N0) * MT, (p - N0 + 1) * MT, nrow, 0)

    def scoped(name, f, i):
        with jax.named_scope(name):
            f(i // 2, i % 2)

    phase(0, U0, pre_piece)
    phase(U0, G0, unit_piece)
    phase(G0, O0, gap_piece)
    phase(O0, N0, lambda p: o_step(p - O0))
    phase(N0, GU0, norm_piece)
    phase(GU0, DN0, lambda p: scoped("gu", gu_part, p - GU0))
    phase(DN0, NP, lambda p: scoped("dn", dn_part, p - DN0))

    def drain(n, cr):
        wait(OST.at[n, :, pl.ds(0, NS - 1)], ossem.at[n])

        @pl.when(n < NFO)
        def _():
            wait(FO.at[n], fossem.at[n])

        return cr

    lax.fori_loop(0, 3 * q4, drain, 0)
    wait(G.at[:, pl.ds(0, (nf - 1) * RD)], gssem)
    for k in classes:
        b, nr = k["buf"], k["nr"]
        wait(b.at[:, :, pl.ds(0, 2), pl.ds(0, nr)], ssem.at[k["ci"], 0])
        wait(b.at[:, :, 1, pl.ds(0, nr)], ssem.at[k["ci"], 1])
        if k["two"]:
            wait(b.at[:, :, :, pl.ds(0, nr)], ssem.at[k["ci"], 2])
        wait(b.at[:, :, :, pl.ds(0, k["R"] // 2)], ssem.at[k["ci"], 3])


def local_layer(x, norm_attn, wq, wk, wv, wo, norm_mlp, wg, wu, wd, *, nf, ns):
    rows, tl, D = x.shape
    F = wg.shape[1]
    nx = ns // 2
    nrb = tl // SUB
    nhg = D // CB
    ngu = -(-F // CB)
    units = 3 * nhg // 2
    rd, rf = D // nf, F // nf
    tok = ns * tl

    idx = np.arange(tok, dtype=np.int32)
    blk, src, low = idx // (ns * SUB), idx % (ns * SUB) // SUB, idx % SUB
    pos = (blk * SUB + low) * ns + src
    inv_freq = np.exp(np.arange(HEAD // 2, dtype=np.float32) * np.float32(-2.0 * math.log(THETA) / HEAD))
    ang = (pos.astype(np.float32)[:, None] * inv_freq[None, :]).astype(np.float64)
    cs, sn = np.cos(ang).astype(np.float32), np.sin(ang).astype(np.float32)
    cos_t = jnp.asarray(np.concatenate([cs, cs], axis=1).reshape(nrb, ns, SUB, HEAD))
    sin_t = jnp.asarray(np.concatenate([-sn, sn], axis=1).reshape(nrb, ns, SUB, HEAD))
    qt = 2 * ns * SUB
    mask_t = jnp.asarray((pos[None, :qt] <= pos[:qt, None]).astype(np.float32))
    x4 = x.reshape(rows, nrb, SUB, D)

    nsteps = nhg * 3 + ngu
    dma = pltpu.SemaphoreType.DMA
    anyspec = pl.BlockSpec(memory_space=pl.ANY)
    vspec = pl.BlockSpec(memory_space=pltpu.VMEM)
    outs = [
        pltpu.VMEM((rows, nrb, SUB, D), BF16),
        jax.ShapeDtypeStruct((nhg, 3, nf - 1, rd, CB), BF16),
        jax.ShapeDtypeStruct((nhg, 1, nf - 1, rd, CB), BF16),
        jax.ShapeDtypeStruct((ngu, 2, nf - 1, rd, CB), BF16),
        jax.ShapeDtypeStruct((nhg, 1, nf - 1, rf, CB), BF16),
    ]
    res = pl.pallas_call(
        functools.partial(kernel, (nf, nx, D, F, rows, nrb, ns)),
        out_shape=outs,
        in_specs=[anyspec] + [vspec] * 5 + [anyspec] * 7,
        out_specs=[vspec] + [anyspec] * 4,
        scratch_shapes=[
            pltpu.VMEM((rows, nrb, SUB, D), BF16),
            pltpu.VMEM((rows, nrb, SUB, F), BF16),
            pltpu.VMEM((units, nrb, ns, SUB, CB), BF16),
            pltpu.VMEM((2, nrb, ns, SUB, CB), BF16),
            pltpu.VMEM((2, nrb, ns, SUB, CB), BF16),
            pltpu.VMEM((2, nrb, ns, SUB, CB), BF16),
            pltpu.VMEM((2, 3, nf, rd, CB), BF16),
            pltpu.VMEM((2, F, CB), BF16),
            pltpu.VMEM((rows // nx, nrb, SUB, D), BF16),
            pltpu.VMEM((units, nrb, 2, SUB, CB), BF16),
            pltpu.VMEM((8, rd), F32),
            pltpu.VMEM((8, D), F32),
            pltpu.VMEM((2, rows, nrb, SUB, CB), BF16),
            pltpu.VMEM((2, nrb, SUB, D), BF16),
            dma((nsteps, 4)),
            dma((4, 4)),
            dma,
            dma,
            dma((3,)),
            dma((nx,)),
            dma,
            dma((rows // nx,)),
            dma,
            dma,
            dma((rows,)),
            dma((units,)),
            dma((units,)),
            dma((units,)),
            dma((2,)),
            dma((2,)),
            dma((2,)),
            dma,
        ],
        compiler_params=pltpu.CompilerParams(collective_id=0, has_side_effects=True, vmem_limit_bytes=58 * 1000 * 1000),
        cost_estimate=pl.CostEstimate(flops=170_000_000_000, bytes_accessed=400_000_000, transcendentals=0),
        name="layer",
    )(x4, norm_attn, norm_mlp, cos_t, sin_t, mask_t, wq, wk, wv, wo, wg, wu, wd)
    return res[0].reshape(rows, tl, D)


def solution(mesh):
    row = P(("dp", "fsdp"), "sp", None)
    wspec = P("fsdp", None)
    gspec = P("fsdp")
    fn = functools.partial(local_layer, nf=mesh.shape["fsdp"], ns=mesh.shape["sp"])
    specs = (row, gspec, wspec, wspec, wspec, wspec, gspec, wspec, wspec, wspec)
    return jax.shard_map(fn, mesh=mesh, in_specs=specs, out_specs=row, check_vma=False)
```
